128 devices in a mesh: tm: 16 (over y, z), port: 8 (over x, core).
Axes of the slice: x: 4, y: 4, z: 4, core: 2. Of those that a mesh axis runs over, the one named last changes fastest.
Arguments:
- voltages: float32 [256, 262144], P('port', 'tm'), may hold values from -6 to 6
- currents: float32 [256, 262144], P('port', 'tm'), may hold values from -0.12 to 0.12
- impedance: float32 [256], P('port'), may hold values from 25 to 100
- freq_index: int32 [2048], replicated, may hold values from 1 to 131071
- window_start: int32 [256], P('port'), may hold values from 0 to 131071
- pairing: int32 [256], P('port'), may hold values from 0 to 255
Outputs:
- scattering: float32 [2, 256, 2048], P(None, 'port', 'tm')
The draws below stay inside these ranges and needn't reach their ends.
All inputs are finite; a program needn't handle non-finite values.
Results may differ from the reference program's by a relative error of at most 0.011.
Values sent between devices are 32-bit elements; how exact they have to be, the bound alone decides.
No kernel may reach another device: no remote copies, remote signals or barrier semaphores. Data moves between devices by JAX's collectives and lax.ppermute only.
A program may use at most 128 MiB of HBM per device.

```python
import math
import jax
import jax.numpy as jnp
from jax import lax

P_SIZE = 256
F = 2048
NT = 262144


def plant(entries, rng, least, top_value):
    spot = [jax.random.randint(jax.random.fold_in(rng, axis), (), 0, length) for axis, length in enumerate(entries.shape)]
    longest = entries.shape.index(max(entries.shape))
    neighbour = spot[:longest] + [(spot[longest] + 1) % entries.shape[longest]] + spot[longest + 1:]
    return entries.at[tuple(spot)].set(least).at[tuple(neighbour)].set(top_value)


def block_levels(own_key, shape, shards, low, largest):
    loudness, own = 1.0, jax.random.fold_in(own_key, 6)
    for axis_at, parts in shards:
        steps = jnp.exp(jax.random.uniform(jax.random.fold_in(own, axis_at), (parts,), jnp.float32, low / len(shards), largest / len(shards)))
        loudness = loudness * jnp.repeat(steps, shape[axis_at] // parts).reshape([-1 if axis == axis_at else 1 for axis in range(len(shape))])
    return loudness


def gaussian(rng, shape, scale, limit, pieces=(), kind=jnp.bfloat16):
    gain = block_levels(rng, shape, pieces, -0.22, 0.18) if pieces else 1.0
    drawn = jax.random.normal(rng, shape, jnp.float32) * scale * gain
    return jnp.minimum(jnp.maximum(drawn, -limit), limit).astype(kind)


def setup_inputs(seed: int = 0) -> dict:
    arg_keys = jax.random.split(jax.random.key(seed), 7)
    voltages = gaussian(arg_keys[0], (P_SIZE, NT), 1.0, 6.0, ((0, 8), (1, 16)), jnp.float32)
    currents = gaussian(arg_keys[1], (P_SIZE, NT), 0.02, 0.12, ((0, 8), (1, 16)), jnp.float32)
    impedance = jnp.clip(jnp.exp(math.log(100.0) - 1.3862944 * jax.random.uniform(arg_keys[2], (P_SIZE,), jnp.float32) ** block_levels(arg_keys[2], (P_SIZE,), ((0, 8),), -0.2, 0.2)), 25.0, 100.0)
    freq_index = plant(jax.random.randint(arg_keys[3], (F,), 1, NT // 2), jax.random.fold_in(arg_keys[3], 1), 1, (NT // 2) - 1).astype(jnp.int32)
    window_start = plant(jax.random.randint(arg_keys[4], (P_SIZE,), 0, NT // 2), jax.random.fold_in(arg_keys[4], 1), 0, (NT // 2) - 1).astype(jnp.int32)
    pairing = plant(jax.random.randint(arg_keys[5], (P_SIZE,), 0, P_SIZE), jax.random.fold_in(arg_keys[5], 1), 0, P_SIZE - 1).astype(jnp.int32)
    return {"voltages": voltages, "currents": currents, "impedance": impedance, "freq_index": freq_index, "window_start": window_start, "pairing": pairing}


def twiddles(freq_index, times, total):
    high = freq_index // 512
    low = freq_index % 512
    stride = times * 512 % total
    phase = (stride[:, None] * high[None, :] % total + times[:, None] * low[None, :]) % total
    angle = phase.astype(jnp.float32) * (2.0 * math.pi / total)
    return jnp.concatenate([jnp.cos(angle), -jnp.sin(angle)], axis=1).astype(jnp.bfloat16)

def waves(spec_v, spec_c, impedance, width):
    zcol = impedance[:, None]
    root = 2.0 * jnp.sqrt(zcol)
    v_re, v_im = (spec_v[:, :width], spec_v[:, width:])
    c_re, c_im = (spec_c[:, :width], spec_c[:, width:])
    a_re = (v_re + zcol * c_re) / root
    a_im = (v_im + zcol * c_im) / root
    b_re = (v_re - zcol * c_re) / root
    b_im = (v_im - zcol * c_im) / root
    return (a_re, a_im, b_re, b_im)

def reference(voltages, currents, impedance, freq_index, window_start, pairing):
    ports, total = voltages.shape
    width = freq_index.shape[0]
    block = math.gcd(total, 8192)
    times_all = jnp.arange(total, dtype=jnp.int32)
    gate = times_all[None, :] >= window_start[:, None]
    gated_v = jnp.where(gate, voltages, 0.0).astype(jnp.bfloat16)
    gated_c = jnp.where(gate, currents, 0.0).astype(jnp.bfloat16)

    def accumulate(carry, index):
        start = index * block
        times = start + jnp.arange(block, dtype=jnp.int32)
        table = twiddles(freq_index, times, total)
        part_v = lax.dynamic_slice_in_dim(gated_v, start, block, 1)
        part_c = lax.dynamic_slice_in_dim(gated_c, start, block, 1)
        return ((carry[0] + jnp.dot(part_v, table, preferred_element_type=jnp.float32), carry[1] + jnp.dot(part_c, table, preferred_element_type=jnp.float32)), None)
    empty = jnp.zeros((ports, 2 * width), jnp.float32)
    (sum_v, sum_c), _ = lax.scan(accumulate, (empty, empty), jnp.arange(total // block, dtype=jnp.int32))
    scale = 1.0 / math.sqrt(total)
    a_re, a_im, b_re, b_im = waves(sum_v * scale, sum_c * scale, impedance, width)
    power = a_re * a_re + a_im * a_im
    mean_power = lax.optimization_barrier(jnp.sum(power, axis=1)) / width + 1e-06
    q_re = jnp.take(a_re, pairing, axis=0)
    q_im = jnp.take(a_im, pairing, axis=0)
    q_power = jnp.take(power, pairing, axis=0)
    q_mean = jnp.take(mean_power, pairing, axis=0)
    denom = jnp.maximum(q_power, 0.1 * q_mean[:, None])
    s_re = (b_re * q_re + b_im * q_im) / denom
    s_im = (b_im * q_re - b_re * q_im) / denom
    return jnp.stack([s_re, s_im], axis=0)
```

```python
import functools
import math

import jax
import jax.numpy as jnp
from jax import lax
from jax.experimental import pallas as pl
from jax.experimental.pallas import tpu as pltpu
from jax.sharding import PartitionSpec as P

LANES = 128
COLUMNS = 256


def turned(phase, total):
    bits = total.bit_length() - 1
    wrapped = phase & (total - 1)
    quarter = (wrapped + total // 8) >> (bits - 2)
    rest = wrapped - (quarter << (bits - 2))
    x = rest.astype(jnp.float32) * (2.0 * math.pi / total)
    y = x * x
    sine = x + x * y * (-1.6666654611e-1 + y * (8.3321608736e-3 - y * 1.9515295891e-4))
    cosine = (
        1.0
        - 0.5 * y
        + y * y * (4.166664568298827e-2 + y * (-1.388731625493765e-3 + y * 2.443315711809948e-5))
    )
    odd = (quarter & 1) == 1
    even_part = jnp.where(odd, sine, cosine)
    odd_part = jnp.where(odd, cosine, sine)
    flip = ((quarter + 1) & 2) == 2
    below = (quarter & 2) == 2
    return jnp.where(flip, -even_part, even_part), jnp.where(below, odd_part, -odd_part)


def as_column(scalars, rows, dtype):
    row = lax.broadcasted_iota(jnp.int32, (rows, LANES), 0)
    column = jnp.zeros((rows, LANES), dtype)
    for r in range(rows):
        column = jnp.where(row == r, scalars[r], column)
    return column


def transform_body(
    first_ref, start_ref, lines_ref, v_ref, c_ref, out_ref, rows_ref, table_ref, *, inner, total
):
    ports, times = v_ref.shape
    both = 2 * ports
    outer = times // inner
    width = lines_ref.shape[1]

    @pl.when(pl.program_id(0) == 0)
    def _():
        start = as_column(start_ref, ports, jnp.int32)[:, :1]
        for s in range(outer):
            at = slice(s * inner, (s + 1) * inner)
            time = first_ref[0] + s * inner + lax.broadcasted_iota(jnp.int32, (ports, inner), 1)
            keep = time >= start
            low = s * both
            rows_ref[low : low + ports] = jnp.where(keep, v_ref[:, at], 0.0).astype(jnp.bfloat16)
            rows_ref[low + ports : low + both] = jnp.where(keep, c_ref[:, at], 0.0).astype(
                jnp.bfloat16
            )

    lines = lines_ref[...]

    def steps(count):
        return lax.broadcasted_iota(jnp.int32, (count, width), 0)

    fine = 16
    coarse = inner // fine
    fine_cos, fine_sin = turned(lines * steps(fine), total)
    coarse_cos, coarse_sin = turned(lines * (steps(coarse) * fine), total)
    outer_cos, outer_sin = turned(lines * (first_ref[0] + steps(outer) * inner), total)
    for u in range(coarse):
        cos_u, sin_u = coarse_cos[u : u + 1], coarse_sin[u : u + 1]
        at = slice(u * fine, (u + 1) * fine)
        table_ref[at, :width] = (cos_u * fine_cos - sin_u * fine_sin).astype(jnp.bfloat16)
        table_ref[at, width:] = (sin_u * fine_cos + cos_u * fine_sin).astype(jnp.bfloat16)
    group = max(1, 512 // both)
    re = jnp.zeros((both, width), jnp.float32)
    im = jnp.zeros((both, width), jnp.float32)
    for g in range(0, outer, group):
        part = jnp.dot(
            rows_ref[g * both : (g + group) * both],
            table_ref[...],
            preferred_element_type=jnp.float32,
        )
        for s in range(group):
            part_re = part[s * both : (s + 1) * both, :width]
            part_im = part[s * both : (s + 1) * both, width:]
            cos_s, sin_s = outer_cos[g + s : g + s + 1], outer_sin[g + s : g + s + 1]
            re = re + (part_re * cos_s - part_im * sin_s)
            im = im + (part_re * sin_s + part_im * cos_s)
    for d in range(width // LANES):
        at = slice(d * LANES, (d + 1) * LANES)
        out_ref[d, :both] = re[:, at]
        out_ref[d, both:] = im[:, at]


def transform(first, start, freq_index, voltages, currents, total):
    ports, times = voltages.shape
    count = freq_index.shape[0]
    inner = min(times, 1024)
    width = min(count, COLUMNS)
    held = pl.BlockSpec((ports, times), lambda i: (0, 0), pipeline_mode=pl.Buffered(1))
    return pl.pallas_call(
        functools.partial(transform_body, inner=inner, total=total),
        grid=(count // width,),
        in_specs=[
            pl.BlockSpec(memory_space=pltpu.SMEM),
            pl.BlockSpec(memory_space=pltpu.SMEM),
            pl.BlockSpec((1, width), lambda i: (0, i)),
            held,
            held,
        ],
        out_specs=pl.BlockSpec((width // LANES, 4 * ports, LANES), lambda i: (i, 0, 0)),
        out_shape=jax.ShapeDtypeStruct((count // LANES, 4 * ports, LANES), jnp.float32),
        scratch_shapes=[
            pltpu.VMEM((times // inner * 2 * ports, inner), jnp.bfloat16),
            pltpu.VMEM((inner, 2 * width), jnp.bfloat16),
        ],
        compiler_params=pltpu.CompilerParams(
            dimension_semantics=("arbitrary",), vmem_limit_bytes=48 << 20
        ),
        name="transform",
    )(first.reshape(1), start, freq_index.reshape(1, count), voltages, currents)


def waves_body(impedance_ref, parts_ref, sent_ref, own_ref, *, scale):
    ports = own_ref.shape[0]
    total = jnp.sum(parts_ref[...], axis=0) * scale
    z = as_column(impedance_ref, ports, jnp.float32)
    inverse = 1.0 / (2.0 * jnp.sqrt(z))
    v_re, c_re = total[:ports], total[ports : 2 * ports]
    v_im, c_im = total[2 * ports : 3 * ports], total[3 * ports :]
    a = jnp.concatenate([(v_re + z * c_re) * inverse, (v_im + z * c_im) * inverse], axis=1)
    own_ref[:, :LANES] = (v_re - z * c_re) * inverse
    own_ref[:, LANES:] = (v_im - z * c_im) * inverse
    for d in range(sent_ref.shape[0]):
        sent_ref[d] = a


def pick_body(pairing_ref, every_ref, own_ref, sent_ref, out_ref, q_ref):
    ports = own_ref.shape[0]
    for p in range(ports):
        q_ref[p : p + 1] = every_ref[pl.ds(pairing_ref[p], 1)]
    q_re, q_im = q_ref[:, :LANES], q_ref[:, LANES:]
    b_re, b_im = own_ref[:, :LANES], own_ref[:, LANES:]
    power = q_re * q_re + q_im * q_im
    out_ref[0] = b_re * q_re + b_im * q_im
    out_ref[1] = b_im * q_re - b_re * q_im
    out_ref[2] = power
    padded = jnp.concatenate([power, jnp.zeros((LANES - ports, LANES), jnp.float32)], axis=0)
    share = jnp.sum(padded.T, axis=0, keepdims=True)
    for d in range(sent_ref.shape[0]):
        sent_ref[d] = jnp.broadcast_to(share, sent_ref.shape[1:])


def divide_body(shares_ref, made_ref, out_ref, *, width):
    ports = out_ref.shape[1]
    summed = jnp.sum(shares_ref[:, 0, :], axis=0, keepdims=True)
    mean = jnp.broadcast_to(summed / width + 1e-06, (LANES, LANES)).T[:ports]
    inverse = 1.0 / jnp.maximum(made_ref[2], 0.1 * mean)
    out_ref[0] = made_ref[0] * inverse
    out_ref[1] = made_ref[1] * inverse


def body(voltages, currents, impedance, freq_index, window_start, pairing):
    ports, times = voltages.shape
    width = freq_index.shape[0]
    times_count, ports_count = lax.axis_size("tm"), lax.axis_size("port")
    total = times * times_count
    first = lax.axis_index("tm") * times
    parts = transform(first, window_start, freq_index, voltages, currents, total)
    parts = lax.all_to_all(parts, "tm", 0, 0, tiled=True)
    smem = pl.BlockSpec(memory_space=pltpu.SMEM)
    vmem = pl.BlockSpec(memory_space=pltpu.VMEM)
    sent, own = pl.pallas_call(
        functools.partial(waves_body, scale=1.0 / math.sqrt(total)),
        in_specs=[smem, vmem],
        out_specs=[vmem, vmem],
        out_shape=[
            jax.ShapeDtypeStruct((ports_count, ports, 2 * LANES), jnp.float32),
            jax.ShapeDtypeStruct((ports, 2 * LANES), jnp.float32),
        ],
        name="waves",
    )(impedance, parts)
    every = lax.all_to_all(sent, "port", 0, 0, tiled=True)
    every = every.reshape(ports_count * ports, 2 * LANES)
    shares, made = pl.pallas_call(
        pick_body,
        in_specs=[smem, vmem, vmem],
        out_specs=[vmem, vmem],
        out_shape=[
            jax.ShapeDtypeStruct((times_count, 8, LANES), jnp.float32),
            jax.ShapeDtypeStruct((3, ports, LANES), jnp.float32),
        ],
        scratch_shapes=[pltpu.VMEM((ports, 2 * LANES), jnp.float32)],
        name="pick",
    )(pairing, every, own)
    shares = lax.all_to_all(shares, "tm", 0, 0, tiled=True)
    return pl.pallas_call(
        functools.partial(divide_body, width=width),
        in_specs=[vmem, vmem],
        out_specs=vmem,
        out_shape=jax.ShapeDtypeStruct((2, ports, LANES), jnp.float32),
        name="divide",
    )(shares, made)


def solution(mesh):
    placed = (P("port", "tm"), P("port", "tm"), P("port"), P(), P("port"), P("port"))
    return jax.shard_map(
        body, mesh=mesh, in_specs=placed, out_specs=P(None, "port", "tm"), check_vma=False
    )
```

```python
import functools
import math

import jax
import jax.numpy as jnp
from jax import lax
from jax.experimental import pallas as pl
from jax.experimental.pallas import tpu as pltpu
from jax.sharding import PartitionSpec as P


LANES = 128
HALF = LANES // 2
COLUMNS = 256
INNER = 1024
SMEM = pl.BlockSpec(memory_space=pltpu.SMEM)
VMEM = pl.BlockSpec(memory_space=pltpu.VMEM)
HBM = pl.BlockSpec(memory_space=pltpu.HBM)


def in_hbm(array):
    return pltpu.with_memory_space_constraint(array, pltpu.HBM)


def in_vmem(array):
    return pltpu.with_memory_space_constraint(array, pltpu.VMEM)


def turned(phase, total):
    bits = total.bit_length() - 1
    wrapped = phase & (total - 1)
    quarter = (wrapped + total // 8) >> (bits - 2)
    rest = wrapped - (quarter << (bits - 2))
    x = rest.astype(jnp.float32) * (2.0 * math.pi / total)
    y = x * x
    sine = x + x * y * (-1.6666654611e-1 + y * (8.3321608736e-3 - y * 1.9515295891e-4))
    cosine = (
        1.0
        - 0.5 * y
        + y * y * (4.166664568298827e-2 + y * (-1.388731625493765e-3 + y * 2.443315711809948e-5))
    )
    odd = (quarter & 1) == 1
    even_part = jnp.where(odd, sine, cosine)
    odd_part = jnp.where(odd, cosine, sine)
    flip = ((quarter + 1) & 2) == 2
    below = (quarter & 2) == 2
    return jnp.where(flip, -even_part, even_part), jnp.where(below, odd_part, -odd_part)


def as_column(scalars, rows, dtype):
    row = lax.broadcasted_iota(jnp.int32, (rows, LANES), 0)
    column = jnp.zeros((rows, LANES), dtype)
    for r in range(rows):
        column = jnp.where(row == r, scalars[r], column)
    return column


def lower(shape):
    return lax.broadcasted_iota(jnp.int32, shape, 1) < HALF


def joined(first, second, which):
    if which == 0:
        return jnp.where(lower(first.shape), first, pltpu.roll(second, HALF, 1))
    return jnp.where(lower(first.shape), pltpu.roll(first, HALF, 1), second)


def add_lines(first_ref, lines_ref, rows_ref, table_ref, out_ref, *, both, inner, total, which):
    outer = rows_ref.shape[0] // both
    tiles = lines_ref.shape[1] // (2 * LANES)
    width = tiles * LANES
    lines = jnp.concatenate(
        [
            joined(
                lines_ref[:, 2 * j * LANES : (2 * j + 1) * LANES],
                lines_ref[:, (2 * j + 1) * LANES : (2 * j + 2) * LANES],
                which,
            )
            for j in range(tiles)
        ],
        axis=1,
    )

    def steps(count):
        return lax.broadcasted_iota(jnp.int32, (count, width), 0)

    fine = 16
    coarse = inner // fine
    fine_cos, fine_sin = turned(lines * steps(fine), total)
    coarse_cos, coarse_sin = turned(lines * (steps(coarse) * fine), total)
    outer_cos, outer_sin = turned(lines * (first_ref[0] + steps(outer) * inner), total)
    for u in range(coarse):
        cos_u, sin_u = coarse_cos[u : u + 1], coarse_sin[u : u + 1]
        at = slice(u * fine, (u + 1) * fine)
        table_ref[at, :width] = (cos_u * fine_cos - sin_u * fine_sin).astype(jnp.bfloat16)
        table_ref[at, width:] = (sin_u * fine_cos + cos_u * fine_sin).astype(jnp.bfloat16)
    yield
    group = max(1, 512 // both)
    re = jnp.zeros((both, width), jnp.float32)
    im = jnp.zeros((both, width), jnp.float32)
    for g in range(0, outer, group):
        part = jnp.dot(
            rows_ref[g * both : (g + group) * both],
            table_ref[...],
            preferred_element_type=jnp.float32,
        )
        for s in range(group):
            part_re = part[s * both : (s + 1) * both, :width]
            part_im = part[s * both : (s + 1) * both, width:]
            cos_s, sin_s = outer_cos[g + s : g + s + 1], outer_sin[g + s : g + s + 1]
            re = re + (part_re * cos_s - part_im * sin_s)
            im = im + (part_re * sin_s + part_im * cos_s)
    for j in range(tiles):
        at = slice(j * LANES, (j + 1) * LANES)
        for h in range(2):
            out_ref[2 * j + h] = joined(re[:, at], im[:, at], h)
    yield


def first_body(
    first_ref, start_ref, lines_ref, v_ref, c_ref, out_ref, rows_ref, table_ref, v_in, c_in, sems,
    *, inner, total
):
    ports, times = v_in.shape
    both = 2 * ports
    outer = times // inner
    begin = pl.program_id(0) == 0

    def copies(s):
        at = pl.ds(s * inner, inner)
        return (
            pltpu.make_async_copy(v_ref.at[:, at], v_in.at[:, at], sems.at[0, s]),
            pltpu.make_async_copy(c_ref.at[:, at], c_in.at[:, at], sems.at[1, s]),
        )

    @pl.when(begin)
    def _():
        for s in range(outer):
            for copy in copies(s):
                copy.start()

    work = add_lines(
        first_ref, lines_ref, rows_ref, table_ref, out_ref,
        both=both, inner=inner, total=total, which=0,
    )
    next(work)

    @pl.when(begin)
    def _():
        start = as_column(start_ref, ports, jnp.int32)[:, :1]
        for s in range(outer):
            at = slice(s * inner, (s + 1) * inner)
            time = first_ref[0] + s * inner + lax.broadcasted_iota(jnp.int32, (ports, inner), 1)
            keep = time >= start
            low = s * both
            for copy in copies(s):
                copy.wait()
            rows_ref[low : low + ports] = jnp.where(keep, v_in[:, at], 0.0).astype(jnp.bfloat16)
            rows_ref[low + ports : low + both] = jnp.where(keep, c_in[:, at], 0.0).astype(
                jnp.bfloat16
            )

    next(work)


def second_body(first_ref, lines_ref, rows_ref, out_ref, table_ref, *, both, inner, total):
    work = add_lines(
        first_ref, lines_ref, rows_ref, table_ref, out_ref,
        both=both, inner=inner, total=total, which=1,
    )
    next(work)
    next(work)


def transforms(first, start, freq_index, voltages, currents, total):
    ports, times = voltages.shape
    both = 2 * ports
    count = freq_index.shape[0]
    inner = min(times, INNER)
    outer = times // inner
    lines = pl.BlockSpec((1, 2 * COLUMNS), lambda i: (0, i))
    grid = (count // (2 * COLUMNS),)
    out_spec = pl.BlockSpec((2 * COLUMNS // LANES, both, LANES), lambda i: (i, 0, 0))
    out_shape = pltpu.VMEM((count // LANES, both, LANES), jnp.float32)
    rows_spec = pl.BlockSpec((outer * both, inner), lambda i: (0, 0), pipeline_mode=pl.Buffered(1))
    rows_shape = pltpu.VMEM((outer * both, inner), jnp.bfloat16)
    table = pltpu.VMEM((inner, 2 * COLUMNS), jnp.bfloat16)
    params = pltpu.CompilerParams(dimension_semantics=("arbitrary",), vmem_limit_bytes=40 << 20)
    cost = pl.CostEstimate(
        flops=2 * both * times * count, transcendentals=0, bytes_accessed=8 * ports * times
    )
    first = first.reshape(1)
    freq_index = freq_index.reshape(1, count)
    out_0, rows = pl.pallas_call(
        functools.partial(first_body, inner=inner, total=total),
        grid=grid,
        in_specs=[SMEM, SMEM, lines, HBM, HBM],
        out_specs=[out_spec, rows_spec],
        out_shape=[out_shape, rows_shape],
        scratch_shapes=[
            table,
            pltpu.VMEM((ports, times), jnp.float32),
            pltpu.VMEM((ports, times), jnp.float32),
            pltpu.SemaphoreType.DMA((2, outer)),
        ],
        compiler_params=params,
        cost_estimate=cost,
        name="spectrum_first",
    )(first, in_hbm(start), in_hbm(freq_index), in_hbm(voltages), in_hbm(currents))
    out_1 = pl.pallas_call(
        functools.partial(second_body, both=both, inner=inner, total=total),
        grid=grid,
        in_specs=[SMEM, lines, rows_spec],
        out_specs=out_spec,
        out_shape=out_shape,
        scratch_shapes=[table],
        compiler_params=params,
        cost_estimate=cost,
        name="spectrum_second",
    )(first, in_hbm(freq_index), in_vmem(rows))
    return out_0, out_1


def waves_body(impedance_ref, parts_ref, sent_ref, own_ref, *, scale):
    ports = own_ref.shape[0]
    total = jnp.sum(parts_ref[...], axis=0) * scale
    z = as_column(impedance_ref, ports, jnp.float32)
    inverse = 1.0 / (2.0 * jnp.sqrt(z))
    v, c = total[:ports], total[ports:]
    a = (v + z * c) * inverse
    own_ref[...] = (v - z * c) * inverse
    for d in range(sent_ref.shape[0]):
        sent_ref[d] = a


def waves(impedance, parts, total, ports_count):
    ports = parts.shape[1] // 2
    return pl.pallas_call(
        functools.partial(waves_body, scale=1.0 / math.sqrt(total)),
        in_specs=[SMEM, VMEM],
        out_specs=[VMEM, VMEM],
        out_shape=[
            pltpu.VMEM((ports_count, ports, LANES), jnp.float32),
            pltpu.VMEM((ports, LANES), jnp.float32),
        ],
        name="waves",
    )(in_hbm(impedance), in_vmem(parts))


def pick_body(pairing_ref, every_0, every_1, own_0, own_1, sent_ref, out_ref, q_ref):
    ports = own_0.shape[0]
    summed = jnp.zeros((ports, LANES), jnp.float32)
    for h, (every_ref, own_ref) in enumerate(((every_0, own_0), (every_1, own_1))):
        for p in range(ports):
            q_ref[h, p : p + 1] = every_ref[pl.ds(pairing_ref[p], 1)]
        q, b = q_ref[h], own_ref[...]
        square = q * q
        summed = summed + square
        same = b * q
        cross = b * pltpu.roll(q, HALF, 1)
        out_ref[h, 0] = jnp.where(
            lower(q.shape), same + pltpu.roll(same, HALF, 1), cross - pltpu.roll(cross, HALF, 1)
        )
        out_ref[h, 1] = square + pltpu.roll(square, HALF, 1)
    padded = jnp.concatenate([summed, jnp.zeros((LANES - ports, LANES), jnp.float32)], axis=0)
    share = jnp.sum(padded.T, axis=0, keepdims=True)
    sent_ref[...] = jnp.broadcast_to(share, sent_ref.shape)


def divide_body(shares_ref, made_ref, out_ref, *, width):
    ports = out_ref.shape[1]
    summed = jnp.sum(shares_ref[...], axis=0, keepdims=True)
    mean = jnp.broadcast_to(summed / width + 1e-06, (LANES, LANES)).T[:ports]
    halves = [made_ref[h, 0] / jnp.maximum(made_ref[h, 1], 0.1 * mean) for h in range(2)]
    for r in range(2):
        out_ref[r] = joined(halves[0], halves[1], r)


def body(voltages, currents, impedance, freq_index, window_start, pairing):
    ports, times = voltages.shape
    width = freq_index.shape[0]
    times_count, ports_count = lax.axis_size("tm"), lax.axis_size("port")
    total = times * times_count
    first = lax.axis_index("tm") * times
    everyone, own = [], []
    halves = transforms(first, window_start, freq_index, voltages, currents, total)
    for parts in halves:
        parts = lax.all_to_all(in_vmem(parts), "tm", 0, 0, tiled=True)
        sent, mine = waves(impedance, parts, total, ports_count)
        every = lax.all_to_all(sent, "port", 0, 0, tiled=True)
        everyone.append(every.reshape(ports_count * ports, LANES))
        own.append(mine)
    shares, made = pl.pallas_call(
        pick_body,
        in_specs=[SMEM, VMEM, VMEM, VMEM, VMEM],
        out_specs=[VMEM, VMEM],
        out_shape=[
            pltpu.VMEM((times_count, LANES), jnp.float32),
            pltpu.VMEM((2, 2, ports, LANES), jnp.float32),
        ],
        scratch_shapes=[pltpu.VMEM((2, ports, LANES), jnp.float32)],
        name="pick",
    )(in_hbm(pairing), *map(in_vmem, everyone), *map(in_vmem, own))
    shares = lax.all_to_all(shares, "tm", 0, 0, tiled=True)
    return pl.pallas_call(
        functools.partial(divide_body, width=width),
        in_specs=[VMEM, VMEM],
        out_specs=VMEM,
        out_shape=jax.ShapeDtypeStruct((2, ports, LANES), jnp.float32),
        name="divide",
    )(in_vmem(shares), in_vmem(made))


def solution(mesh):
    placed = (P("port", "tm"), P("port", "tm"), P("port"), P(), P("port"), P("port"))
    return jax.shard_map(
        body, mesh=mesh, in_specs=placed, out_specs=P(None, "port", "tm"), check_vma=False
    )
```

```python
import functools
import math

import jax
import jax.numpy as jnp
from jax import lax
from jax.experimental import pallas as pl
from jax.experimental.pallas import tpu as pltpu
from jax.sharding import PartitionSpec as P

LANES = 128
COLUMNS = 256
INNER = 1024
FLIP = 256
SMEM = pl.BlockSpec(memory_space=pltpu.SMEM)
VMEM = pl.BlockSpec(memory_space=pltpu.VMEM)
HBM = pl.BlockSpec(memory_space=pltpu.HBM)


def in_hbm(array):
    return pltpu.with_memory_space_constraint(array, pltpu.HBM)


def in_vmem(array):
    return pltpu.with_memory_space_constraint(array, pltpu.VMEM)


def turned(phase, total):
    bits = total.bit_length() - 1
    wrapped = phase & (total - 1)
    quarter = (wrapped + total // 8) >> (bits - 2)
    rest = wrapped - (quarter << (bits - 2))
    x = rest.astype(jnp.float32) * (2.0 * math.pi / total)
    y = x * x
    sine = x + x * y * (-1.6666654611e-1 + y * (8.3321608736e-3 - y * 1.9515295891e-4))
    cosine = (
        1.0
        - 0.5 * y
        + y * y * (4.166664568298827e-2 + y * (-1.388731625493765e-3 + y * 2.443315711809948e-5))
    )
    odd = (quarter & 1) == 1
    even_part = jnp.where(odd, sine, cosine)
    odd_part = jnp.where(odd, cosine, sine)
    flip = ((quarter + 1) & 2) == 2
    below = (quarter & 2) == 2
    return jnp.where(flip, -even_part, even_part), jnp.where(below, odd_part, -odd_part)


def as_column(scalars, rows, dtype):
    row = lax.broadcasted_iota(jnp.int32, (rows, LANES), 0)
    column = jnp.zeros((rows, LANES), dtype)
    for r in range(rows):
        column = jnp.where(row == r, scalars[r], column)
    return column


def transform_body(
    first_ref, start_ref, lines_ref, after_ref, v_ref, c_ref, out_ref,
    even_ref, odd_ref, raw_ref, cos_0, sin_0, cos_1, sin_1, turn_0, turn_1, v_in, c_in, sems,
    *, inner, total
):
    ports, times = v_ref.shape
    both = 2 * ports
    outer = times // inner
    half = inner // 2
    cols = lines_ref.shape[1] // 2

    def copies(s):
        at = pl.ds(s * inner, inner)
        return (
            pltpu.make_async_copy(v_ref.at[:, at], v_in.at[:, at], sems.at[0, s]),
            pltpu.make_async_copy(c_ref.at[:, at], c_in.at[:, at], sems.at[1, s]),
        )

    def build(lines, cos_ref, sin_ref, turn_ref):
        def steps(count):
            return lax.broadcasted_iota(jnp.int32, (count, cols), 0)

        fine = 16
        coarse = half // fine
        fine_cos, fine_sin = turned(lines * (2 * steps(fine) + 1), 2 * total)
        coarse_cos, coarse_sin = turned(lines * (steps(coarse) * (2 * fine)), 2 * total)
        middle = 2 * (first_ref[0] + steps(outer) * inner + half) - 1
        turn_ref[:outer], turn_ref[outer:] = turned(lines * middle, 2 * total)
        for u in range(coarse):
            cos_u, sin_u = coarse_cos[u : u + 1], coarse_sin[u : u + 1]
            at = slice(u * fine, (u + 1) * fine)
            cos_ref[at] = (cos_u * fine_cos - sin_u * fine_sin).astype(jnp.bfloat16)
            sin_ref[at] = (sin_u * fine_cos + cos_u * fine_sin).astype(jnp.bfloat16)

    def spectra(cos_ref, sin_ref, turn_ref, base):
        group = max(1, 512 // both)
        re = jnp.zeros((both, cols), jnp.float32)
        im = jnp.zeros((both, cols), jnp.float32)
        for g in range(0, outer, group):
            at = slice(g * both, (g + group) * both)
            part_re = jnp.dot(even_ref[at], cos_ref[...], preferred_element_type=jnp.float32)
            part_im = jnp.dot(odd_ref[at], sin_ref[...], preferred_element_type=jnp.float32)
            for s in range(group):
                re_s = part_re[s * both : (s + 1) * both]
                im_s = part_im[s * both : (s + 1) * both]
                cos_s = turn_ref[g + s : g + s + 1]
                sin_s = turn_ref[outer + g + s : outer + g + s + 1]
                re = re + (re_s * cos_s - im_s * sin_s)
                im = im + (re_s * sin_s + im_s * cos_s)
        for j in range(cols // LANES):
            at = slice(j * LANES, (j + 1) * LANES)
            out_ref[base + j, :both] = re[:, at]
            out_ref[base + j, both:] = im[:, at]

    @pl.when(pl.program_id(0) == 0)
    def _():
        for s in range(outer):
            for copy in copies(s):
                copy.start()
        build(lines_ref[:, :cols], cos_0, sin_0, turn_0)
        start = as_column(start_ref, ports, jnp.int32)[:, :1]
        row = lax.broadcasted_iota(jnp.int32, (FLIP, FLIP), 0)
        col = lax.broadcasted_iota(jnp.int32, (FLIP, FLIP), 1)
        flip = jnp.where(row + col == FLIP - 1, 1.0, 0.0).astype(jnp.bfloat16)
        group = max(1, 256 // both)
        for g in range(0, outer, group):
            for s in range(g, g + group):
                at = slice(s * inner, (s + 1) * inner)
                time = first_ref[0] + s * inner
                time = time + lax.broadcasted_iota(jnp.int32, (ports, inner), 1)
                keep = time >= start
                low = s * both
                for copy in copies(s):
                    copy.wait()
                raw_ref[low : low + ports] = jnp.where(keep, v_in[:, at], 0.0).astype(jnp.bfloat16)
                raw_ref[low + ports : low + both] = jnp.where(keep, c_in[:, at], 0.0).astype(
                    jnp.bfloat16
                )
            at = slice(g * both, (g + group) * both)
            for q in range(half // FLIP):
                to = slice(q * FLIP, (q + 1) * FLIP)
                behind = jnp.dot(
                    raw_ref[at, half - (q + 1) * FLIP : half - q * FLIP],
                    flip,
                    preferred_element_type=jnp.float32,
                )
                ahead = raw_ref[at, half + q * FLIP : half + (q + 1) * FLIP].astype(jnp.float32)
                even_ref[at, to] = (ahead + behind).astype(jnp.bfloat16)
                odd_ref[at, to] = (ahead - behind).astype(jnp.bfloat16)

    build(lines_ref[:, cols:], cos_1, sin_1, turn_1)
    spectra(cos_0, sin_0, turn_0, 0)
    build(after_ref[:, :cols], cos_0, sin_0, turn_0)
    spectra(cos_1, sin_1, turn_1, cols // LANES)


def transform(first, start, freq_index, voltages, currents, total):
    ports, times = voltages.shape
    both = 2 * ports
    count = freq_index.shape[0]
    outer = times // INNER
    half = INNER // 2
    steps = count // (2 * COLUMNS)
    table = pltpu.VMEM((half, COLUMNS), jnp.bfloat16)
    turn = pltpu.VMEM((2 * outer, COLUMNS), jnp.float32)
    lines = in_hbm(freq_index.reshape(1, count))
    return pl.pallas_call(
        functools.partial(transform_body, inner=INNER, total=total),
        grid=(steps,),
        in_specs=[
            SMEM,
            SMEM,
            pl.BlockSpec((1, 2 * COLUMNS), lambda i: (0, i)),
            pl.BlockSpec((1, 2 * COLUMNS), lambda i: (0, jnp.minimum(i + 1, steps - 1))),
            HBM,
            HBM,
        ],
        out_specs=pl.BlockSpec((2 * COLUMNS // LANES, 2 * both, LANES), lambda i: (i, 0, 0)),
        out_shape=pltpu.VMEM((count // LANES, 2 * both, LANES), jnp.float32),
        scratch_shapes=[
            pltpu.VMEM((outer * both, half), jnp.bfloat16),
            pltpu.VMEM((outer * both, half), jnp.bfloat16),
            pltpu.VMEM((outer * both, INNER), jnp.bfloat16),
            table,
            table,
            table,
            table,
            turn,
            turn,
            pltpu.VMEM((ports, times), jnp.float32),
            pltpu.VMEM((ports, times), jnp.float32),
            pltpu.SemaphoreType.DMA((2, outer)),
        ],
        compiler_params=pltpu.CompilerParams(
            dimension_semantics=("arbitrary",), vmem_limit_bytes=48 << 20
        ),
        name="spectrum",
    )(first.reshape(1), in_hbm(start), lines, lines, in_hbm(voltages), in_hbm(currents))


def waves_body(impedance_ref, parts_ref, sent_ref, own_ref, *, scale):
    ports = own_ref.shape[0]
    total = jnp.sum(parts_ref[...], axis=0) * scale
    z = as_column(impedance_ref, ports, jnp.float32)
    inverse = 1.0 / (2.0 * jnp.sqrt(z))
    for r in range(2):
        at = slice(r * LANES, (r + 1) * LANES)
        v = total[2 * r * ports : (2 * r + 1) * ports]
        c = total[(2 * r + 1) * ports : (2 * r + 2) * ports]
        a = (v + z * c) * inverse
        own_ref[:, at] = (v - z * c) * inverse
        for d in range(sent_ref.shape[0]):
            sent_ref[d, :, at] = a


def pick_body(pairing_ref, every_ref, own_ref, sent_ref, made_ref, q_ref):
    ports = own_ref.shape[0]
    for p in range(ports):
        q = pairing_ref[p]
        q_ref[p : p + 1] = every_ref[q // ports, pl.ds(q % ports, 1)]
    q_re, q_im = q_ref[:, :LANES], q_ref[:, LANES:]
    b_re, b_im = own_ref[:, :LANES], own_ref[:, LANES:]
    power = q_re * q_re + q_im * q_im
    made_ref[0] = b_re * q_re + b_im * q_im
    made_ref[1] = b_im * q_re - b_re * q_im
    made_ref[2] = power
    padded = jnp.concatenate([power, jnp.zeros((LANES - ports, LANES), jnp.float32)], axis=0)
    share = jnp.sum(padded.T, axis=0, keepdims=True)
    sent_ref[...] = jnp.broadcast_to(share, sent_ref.shape)


def divide_body(shares_ref, made_ref, out_ref, *, width):
    ports = out_ref.shape[1]
    summed = jnp.sum(shares_ref[...], axis=0, keepdims=True)
    mean = jnp.broadcast_to(summed / width + 1e-06, (LANES, LANES)).T[:ports]
    inverse = 1.0 / jnp.maximum(made_ref[2], 0.1 * mean)
    out_ref[0] = made_ref[0] * inverse
    out_ref[1] = made_ref[1] * inverse


def body(voltages, currents, impedance, freq_index, window_start, pairing):
    ports, times = voltages.shape
    width = freq_index.shape[0]
    times_count, ports_count = lax.axis_size("tm"), lax.axis_size("port")
    total = times * times_count
    first = lax.axis_index("tm") * times
    parts = transform(first, window_start, freq_index, voltages, currents, total)
    parts = lax.all_to_all(in_vmem(parts), "tm", 0, 0, tiled=True)
    sent, own = pl.pallas_call(
        functools.partial(waves_body, scale=1.0 / math.sqrt(total)),
        in_specs=[SMEM, VMEM],
        out_specs=[VMEM, VMEM],
        out_shape=[
            pltpu.VMEM((ports_count, ports, 2 * LANES), jnp.float32),
            pltpu.VMEM((ports, 2 * LANES), jnp.float32),
        ],
        name="waves",
    )(in_hbm(impedance), in_vmem(parts))
    every = lax.all_to_all(in_vmem(sent), "port", 0, 0, tiled=True)
    shares, made = pl.pallas_call(
        pick_body,
        in_specs=[SMEM, VMEM, VMEM],
        out_specs=[VMEM, VMEM],
        out_shape=[
            pltpu.VMEM((times_count, LANES), jnp.float32),
            pltpu.VMEM((3, ports, LANES), jnp.float32),
        ],
        scratch_shapes=[pltpu.VMEM((ports, 2 * LANES), jnp.float32)],
        name="pick",
    )(in_hbm(pairing), in_vmem(every), in_vmem(own))
    shares = lax.all_to_all(in_vmem(shares), "tm", 0, 0, tiled=True)
    return pl.pallas_call(
        functools.partial(divide_body, width=width),
        in_specs=[VMEM, VMEM],
        out_specs=VMEM,
        out_shape=jax.ShapeDtypeStruct((2, ports, LANES), jnp.float32),
        name="divide",
    )(in_vmem(shares), in_vmem(made))


def solution(mesh):
    placed = (P("port", "tm"), P("port", "tm"), P("port"), P(), P("port"), P("port"))
    return jax.shard_map(
        body, mesh=mesh, in_specs=placed, out_specs=P(None, "port", "tm"), check_vma=False
    )
```

```python
import functools
import math

import jax
import jax.numpy as jnp
from jax import lax
from jax.experimental import pallas as pl
from jax.experimental.pallas import tpu as pltpu
from jax.sharding import PartitionSpec as P

LANES = 128
COLUMNS = 256
INNER = 1024
FLIP = 256
SMEM = pl.BlockSpec(memory_space=pltpu.SMEM)
VMEM = pl.BlockSpec(memory_space=pltpu.VMEM)
HBM = pl.BlockSpec(memory_space=pltpu.HBM)


def in_hbm(array):
    return pltpu.with_memory_space_constraint(array, pltpu.HBM)


def in_vmem(array):
    return pltpu.with_memory_space_constraint(array, pltpu.VMEM)


def turned(phase, total):
    bits = total.bit_length() - 1
    wrapped = phase & (total - 1)
    quarter = (wrapped + total // 8) >> (bits - 2)
    rest = wrapped - (quarter << (bits - 2))
    x = rest.astype(jnp.float32) * (2.0 * math.pi / total)
    y = x * x
    sine = x + x * y * (-1.6666654611e-1 + y * (8.3321608736e-3 - y * 1.9515295891e-4))
    cosine = (
        1.0
        - 0.5 * y
        + y * y * (4.166664568298827e-2 + y * (-1.388731625493765e-3 + y * 2.443315711809948e-5))
    )
    odd = (quarter & 1) == 1
    even_part = jnp.where(odd, sine, cosine)
    odd_part = jnp.where(odd, cosine, sine)
    flip = ((quarter + 1) & 2) == 2
    below = (quarter & 2) == 2
    return jnp.where(flip, -even_part, even_part), jnp.where(below, odd_part, -odd_part)


def as_column(scalars, rows, dtype):
    row = lax.broadcasted_iota(jnp.int32, (rows, LANES), 0)
    column = jnp.zeros((rows, LANES), dtype)
    for r in range(rows):
        column = jnp.where(row == r, scalars[r], column)
    return column


def transform_body(
    first_ref, start_ref, lines_ref, after_ref, v_ref, c_ref, out_ref,
    even_ref, odd_ref, raw_ref, cos_0, sin_0, cos_1, sin_1, turn_0, turn_1, v_in, c_in, sems,
    *, inner, total
):
    ports, times = v_ref.shape
    both = 2 * ports
    outer = times // inner
    half = inner // 2
    cols = lines_ref.shape[1] // 2

    def copies(s):
        at = pl.ds(s * inner, inner)
        return (
            pltpu.make_async_copy(v_ref.at[:, at], v_in.at[:, at], sems.at[0, s]),
            pltpu.make_async_copy(c_ref.at[:, at], c_in.at[:, at], sems.at[1, s]),
        )

    def build(lines, cos_ref, sin_ref, turn_ref):
        def steps(count):
            return lax.broadcasted_iota(jnp.int32, (count, cols), 0)

        fine = 16
        coarse = half // fine
        fine_cos, fine_sin = turned(lines * (2 * steps(fine) + 1), 2 * total)
        coarse_cos, coarse_sin = turned(lines * (steps(coarse) * (2 * fine)), 2 * total)
        middle = 2 * (first_ref[0] + steps(outer) * inner + half) - 1
        turn_ref[:outer], turn_ref[outer:] = turned(lines * middle, 2 * total)
        for u in range(coarse):
            cos_u, sin_u = coarse_cos[u : u + 1], coarse_sin[u : u + 1]
            at = slice(u * fine, (u + 1) * fine)
            cos_ref[at] = (cos_u * fine_cos - sin_u * fine_sin).astype(jnp.bfloat16)
            sin_ref[at] = (sin_u * fine_cos + cos_u * fine_sin).astype(jnp.bfloat16)

    def spectra(cos_ref, sin_ref, turn_ref, base):
        group = max(1, 512 // both)
        re = jnp.zeros((both, cols), jnp.float32)
        im = jnp.zeros((both, cols), jnp.float32)
        for g in range(0, outer, group):
            at = slice(g * both, (g + group) * both)
            part_re = jnp.dot(even_ref[at], cos_ref[...], preferred_element_type=jnp.float32)
            part_im = jnp.dot(odd_ref[at], sin_ref[...], preferred_element_type=jnp.float32)
            for s in range(group):
                re_s = part_re[s * both : (s + 1) * both]
                im_s = part_im[s * both : (s + 1) * both]
                cos_s = turn_ref[g + s : g + s + 1]
                sin_s = turn_ref[outer + g + s : outer + g + s + 1]
                re = re + (re_s * cos_s - im_s * sin_s)
                im = im + (re_s * sin_s + im_s * cos_s)
        for j in range(cols // LANES):
            at = slice(j * LANES, (j + 1) * LANES)
            out_ref[base + j, :both] = re[:, at]
            out_ref[base + j, both:] = im[:, at]

    @pl.when(pl.program_id(0) == 0)
    def _():
        for s in range(outer):
            for copy in copies(s):
                copy.start()
        build(lines_ref[:, :cols], cos_0, sin_0, turn_0)
        start = as_column(start_ref, ports, jnp.int32)[:, :1]
        row = lax.broadcasted_iota(jnp.int32, (FLIP, FLIP), 0)
        col = lax.broadcasted_iota(jnp.int32, (FLIP, FLIP), 1)
        flip = jnp.where(row + col == FLIP - 1, 1.0, 0.0).astype(jnp.bfloat16)
        group = max(1, 256 // both)
        for g in range(0, outer, group):
            for s in range(g, g + group):
                at = slice(s * inner, (s + 1) * inner)
                time = first_ref[0] + s * inner
                time = time + lax.broadcasted_iota(jnp.int32, (ports, inner), 1)
                keep = time >= start
                low = s * both
                for copy in copies(s):
                    copy.wait()
                raw_ref[low : low + ports] = jnp.where(keep, v_in[:, at], 0.0).astype(jnp.bfloat16)
                raw_ref[low + ports : low + both] = jnp.where(keep, c_in[:, at], 0.0).astype(
                    jnp.bfloat16
                )
            at = slice(g * both, (g + group) * both)
            for q in range(half // FLIP):
                to = slice(q * FLIP, (q + 1) * FLIP)
                behind = jnp.dot(
                    raw_ref[at, half - (q + 1) * FLIP : half - q * FLIP],
                    flip,
                    preferred_element_type=jnp.float32,
                )
                ahead = raw_ref[at, half + q * FLIP : half + (q + 1) * FLIP].astype(jnp.float32)
                even_ref[at, to] = (ahead + behind).astype(jnp.bfloat16)
                odd_ref[at, to] = (ahead - behind).astype(jnp.bfloat16)

    build(lines_ref[:, cols:], cos_1, sin_1, turn_1)
    spectra(cos_0, sin_0, turn_0, 0)
    build(after_ref[:, :cols], cos_0, sin_0, turn_0)
    spectra(cos_1, sin_1, turn_1, cols // LANES)


def transform(first, start, freq_index, voltages, currents, total):
    ports, times = voltages.shape
    both = 2 * ports
    count = freq_index.shape[0]
    outer = times // INNER
    half = INNER // 2
    steps = count // (2 * COLUMNS)
    table = pltpu.VMEM((half, COLUMNS), jnp.bfloat16)
    turn = pltpu.VMEM((2 * outer, COLUMNS), jnp.float32)
    lines = in_hbm(freq_index.reshape(1, count))
    return pl.pallas_call(
        functools.partial(transform_body, inner=INNER, total=total),
        grid=(steps,),
        in_specs=[
            SMEM,
            SMEM,
            pl.BlockSpec((1, 2 * COLUMNS), lambda i: (0, i)),
            pl.BlockSpec((1, 2 * COLUMNS), lambda i: (0, jnp.minimum(i + 1, steps - 1))),
            HBM,
            HBM,
        ],
        out_specs=pl.BlockSpec((2 * COLUMNS // LANES, 2 * both, LANES), lambda i: (i, 0, 0)),
        out_shape=pltpu.VMEM((count // LANES, 2 * both, LANES), jnp.float32),
        scratch_shapes=[
            pltpu.VMEM((outer * both, half), jnp.bfloat16),
            pltpu.VMEM((outer * both, half), jnp.bfloat16),
            pltpu.VMEM((outer * both, INNER), jnp.bfloat16),
            table,
            table,
            table,
            table,
            turn,
            turn,
            pltpu.VMEM((ports, times), jnp.float32),
            pltpu.VMEM((ports, times), jnp.float32),
            pltpu.SemaphoreType.DMA((2, outer)),
        ],
        compiler_params=pltpu.CompilerParams(
            dimension_semantics=("arbitrary",), vmem_limit_bytes=48 << 20
        ),
        name="spectrum",
    )(first.reshape(1), in_hbm(start), lines, lines, in_hbm(voltages), in_hbm(currents))


def waves_body(impedance_ref, parts_ref, sent_ref, own_ref, *, scale):
    ports = own_ref.shape[0]
    total = jnp.sum(parts_ref[...], axis=0) * scale
    z = as_column(impedance_ref, ports, jnp.float32)
    inverse = 1.0 / (2.0 * jnp.sqrt(z))
    for r in range(2):
        at = slice(r * LANES, (r + 1) * LANES)
        v = total[2 * r * ports : (2 * r + 1) * ports]
        c = total[(2 * r + 1) * ports : (2 * r + 2) * ports]
        sent_ref[:, at] = (v + z * c) * inverse
        own_ref[:, at] = (v - z * c) * inverse


def pick_body(
    place_ref, pairing_ref, pair_0, pair_1, pair_2, pair_3, own_ref, sent_ref, made_ref, every_ref,
    q_ref,
):
    ports = own_ref.shape[0]
    pairs = (pair_0, pair_1, pair_2, pair_3)
    for k, pair in enumerate(pairs):
        every_ref[k] = pair[...]
    for p in range(ports):
        q = pairing_ref[p]
        holder = q // ports
        back = (place_ref[0] // 2 - holder // 2) & (len(pairs) - 1)
        other = (place_ref[0] ^ holder) & 1
        q_ref[p : p + 1] = every_ref[back, other, pl.ds(q % ports, 1)]
    q_re, q_im = q_ref[:, :LANES], q_ref[:, LANES:]
    b_re, b_im = own_ref[:, :LANES], own_ref[:, LANES:]
    power = q_re * q_re + q_im * q_im
    made_ref[0] = b_re * q_re + b_im * q_im
    made_ref[1] = b_im * q_re - b_re * q_im
    made_ref[2] = power
    padded = jnp.concatenate([power, jnp.zeros((LANES - ports, LANES), jnp.float32)], axis=0)
    share = jnp.sum(padded.T, axis=0, keepdims=True)
    sent_ref[...] = jnp.broadcast_to(share, sent_ref.shape)


def divide_body(shares_ref, made_ref, out_ref, *, width):
    ports = out_ref.shape[1]
    summed = jnp.sum(shares_ref[...], axis=0, keepdims=True)
    mean = jnp.broadcast_to(summed / width + 1e-06, (LANES, LANES)).T[:ports]
    inverse = 1.0 / jnp.maximum(made_ref[2], 0.1 * mean)
    out_ref[0] = made_ref[0] * inverse
    out_ref[1] = made_ref[1] * inverse


def body(voltages, currents, impedance, freq_index, window_start, pairing):
    ports, times = voltages.shape
    width = freq_index.shape[0]
    times_count, ports_count = lax.axis_size("tm"), lax.axis_size("port")
    total = times * times_count
    first = lax.axis_index("tm") * times
    parts = transform(first, window_start, freq_index, voltages, currents, total)
    parts = lax.all_to_all(in_vmem(parts), "tm", 0, 0, tiled=True)
    sent, own = pl.pallas_call(
        functools.partial(waves_body, scale=1.0 / math.sqrt(total)),
        in_specs=[SMEM, VMEM],
        out_specs=[VMEM, VMEM],
        out_shape=[
            pltpu.VMEM((ports, 2 * LANES), jnp.float32),
            pltpu.VMEM((ports, 2 * LANES), jnp.float32),
        ],
        name="waves",
    )(in_hbm(impedance), in_vmem(parts))
    swap = [(i, i ^ 1) for i in range(ports_count)]
    pair = jnp.stack([sent, lax.ppermute(sent, "port", swap)])
    pairs = [pair]
    for k in range(1, ports_count // 2):
        ahead = [(i, (i + 2 * k) % ports_count) for i in range(ports_count)]
        pairs.append(lax.ppermute(pair, "port", ahead))
    shares, made = pl.pallas_call(
        pick_body,
        in_specs=[SMEM, SMEM, VMEM, VMEM, VMEM, VMEM, VMEM],
        out_specs=[VMEM, VMEM],
        out_shape=[
            pltpu.VMEM((times_count, LANES), jnp.float32),
            pltpu.VMEM((3, ports, LANES), jnp.float32),
        ],
        scratch_shapes=[
            pltpu.VMEM((ports_count // 2, 2, ports, 2 * LANES), jnp.float32),
            pltpu.VMEM((ports, 2 * LANES), jnp.float32),
        ],
        name="pick",
    )(lax.axis_index("port").reshape(1), in_hbm(pairing), *map(in_vmem, pairs), in_vmem(own))
    shares = lax.all_to_all(in_vmem(shares), "tm", 0, 0, tiled=True)
    return pl.pallas_call(
        functools.partial(divide_body, width=width),
        in_specs=[VMEM, VMEM],
        out_specs=VMEM,
        out_shape=jax.ShapeDtypeStruct((2, ports, LANES), jnp.float32),
        name="divide",
    )(in_vmem(shares), in_vmem(made))


def solution(mesh):
    placed = (P("port", "tm"), P("port", "tm"), P("port"), P(), P("port"), P("port"))
    return jax.shard_map(
        body, mesh=mesh, in_specs=placed, out_specs=P(None, "port", "tm"), check_vma=False
    )
```

```python
import functools
import math

import jax
import jax.numpy as jnp
from jax import lax
from jax.experimental import pallas as pl
from jax.experimental.pallas import tpu as pltpu
from jax.sharding import PartitionSpec as P


LANES = 128
COLUMNS = 256
INNER = 1024
FLIP = 256
SMEM = pl.BlockSpec(memory_space=pltpu.SMEM)
VMEM = pl.BlockSpec(memory_space=pltpu.VMEM)
HBM = pl.BlockSpec(memory_space=pltpu.HBM)


def in_hbm(array):
    return pltpu.with_memory_space_constraint(array, pltpu.HBM)


def in_vmem(array):
    return pltpu.with_memory_space_constraint(array, pltpu.VMEM)


def turned(phase, total):
    bits = total.bit_length() - 1
    wrapped = phase & (total - 1)
    quarter = (wrapped + total // 8) >> (bits - 2)
    rest = wrapped - (quarter << (bits - 2))
    x = rest.astype(jnp.float32) * (2.0 * math.pi / total)
    y = x * x
    sine = x + x * y * (-1.6666654611e-1 + y * (8.3321608736e-3 - y * 1.9515295891e-4))
    cosine = (
        1.0
        - 0.5 * y
        + y * y * (4.166664568298827e-2 + y * (-1.388731625493765e-3 + y * 2.443315711809948e-5))
    )
    odd = (quarter & 1) == 1
    even_part = jnp.where(odd, sine, cosine)
    odd_part = jnp.where(odd, cosine, sine)
    flip = ((quarter + 1) & 2) == 2
    below = (quarter & 2) == 2
    return jnp.where(flip, -even_part, even_part), jnp.where(below, odd_part, -odd_part)


def as_column(scalars, rows, dtype):
    row = lax.broadcasted_iota(jnp.int32, (rows, LANES), 0)
    column = jnp.zeros((rows, LANES), dtype)
    for r in range(rows):
        column = jnp.where(row == r, scalars[r], column)
    return column


def transform_body(
    first_ref, start_ref, lines_ref, after_ref, v_ref, c_ref, out_ref,
    even_ref, odd_ref, raw_ref, cos_0, sin_0, cos_1, sin_1, turn_0, turn_1, v_in, c_in, sems,
    *, inner, total
):
    ports, times = v_ref.shape
    both = 2 * ports
    outer = times // inner
    half = inner // 2
    cols = lines_ref.shape[1] // 2

    def copies(s):
        at = pl.ds(s * inner, inner)
        return (
            pltpu.make_async_copy(v_ref.at[:, at], v_in.at[:, at], sems.at[0, s]),
            pltpu.make_async_copy(c_ref.at[:, at], c_in.at[:, at], sems.at[1, s]),
        )

    def build(lines, cos_ref, sin_ref, turn_ref):
        def steps(count):
            return lax.broadcasted_iota(jnp.int32, (count, cols), 0)

        fine = 16
        coarse = half // fine
        fine_cos, fine_sin = turned(lines * (2 * steps(fine) + 1), 2 * total)
        coarse_cos, coarse_sin = turned(lines * (steps(coarse) * (2 * fine)), 2 * total)
        middle = 2 * (first_ref[0] + steps(outer) * inner + half) - 1
        turn_ref[:outer], turn_ref[outer:] = turned(lines * middle, 2 * total)
        for u in range(coarse):
            cos_u, sin_u = coarse_cos[u : u + 1], coarse_sin[u : u + 1]
            at = slice(u * fine, (u + 1) * fine)
            cos_ref[at] = (cos_u * fine_cos - sin_u * fine_sin).astype(jnp.bfloat16)
            sin_ref[at] = (sin_u * fine_cos + cos_u * fine_sin).astype(jnp.bfloat16)

    def spectra(cos_ref, sin_ref, turn_ref, base):
        group = max(1, 512 // both)
        re = jnp.zeros((both, cols), jnp.float32)
        im = jnp.zeros((both, cols), jnp.float32)
        for g in range(0, outer, group):
            at = slice(g * both, (g + group) * both)
            part_re = jnp.dot(even_ref[at], cos_ref[...], preferred_element_type=jnp.float32)
            part_im = jnp.dot(odd_ref[at], sin_ref[...], preferred_element_type=jnp.float32)
            for s in range(group):
                re_s = part_re[s * both : (s + 1) * both]
                im_s = part_im[s * both : (s + 1) * both]
                cos_s = turn_ref[g + s : g + s + 1]
                sin_s = turn_ref[outer + g + s : outer + g + s + 1]
                re = re + (re_s * cos_s - im_s * sin_s)
                im = im + (re_s * sin_s + im_s * cos_s)
        for j in range(cols // LANES):
            at = slice(j * LANES, (j + 1) * LANES)
            out_ref[base + j, :both] = re[:, at]
            out_ref[base + j, both:] = im[:, at]

    @pl.when(pl.program_id(0) == 0)
    def _():
        for s in range(outer):
            for copy in copies(s):
                copy.start()
        build(lines_ref[:, :cols], cos_0, sin_0, turn_0)
        start = as_column(start_ref, ports, jnp.int32)[:, :1]
        row = lax.broadcasted_iota(jnp.int32, (FLIP, FLIP), 0)
        col = lax.broadcasted_iota(jnp.int32, (FLIP, FLIP), 1)
        flip = jnp.where(row + col == FLIP - 1, 1.0, 0.0).astype(jnp.bfloat16)
        group = max(1, 256 // both)
        for g in range(0, outer, group):
            for s in range(g, g + group):
                at = slice(s * inner, (s + 1) * inner)
                time = first_ref[0] + s * inner
                time = time + lax.broadcasted_iota(jnp.int32, (ports, inner), 1)
                keep = time >= start
                low = s * both
                for copy in copies(s):
                    copy.wait()
                raw_ref[low : low + ports] = jnp.where(keep, v_in[:, at], 0.0).astype(jnp.bfloat16)
                raw_ref[low + ports : low + both] = jnp.where(keep, c_in[:, at], 0.0).astype(
                    jnp.bfloat16
                )
            at = slice(g * both, (g + group) * both)
            for q in range(half // FLIP):
                to = slice(q * FLIP, (q + 1) * FLIP)
                behind = jnp.dot(
                    raw_ref[at, half - (q + 1) * FLIP : half - q * FLIP],
                    flip,
                    preferred_element_type=jnp.float32,
                )
                ahead = raw_ref[at, half + q * FLIP : half + (q + 1) * FLIP].astype(jnp.float32)
                even_ref[at, to] = (ahead + behind).astype(jnp.bfloat16)
                odd_ref[at, to] = (ahead - behind).astype(jnp.bfloat16)

    build(lines_ref[:, cols:], cos_1, sin_1, turn_1)
    spectra(cos_0, sin_0, turn_0, 0)
    build(after_ref[:, :cols], cos_0, sin_0, turn_0)
    spectra(cos_1, sin_1, turn_1, cols // LANES)


def transform(first, start, freq_index, voltages, currents, total):
    ports, times = voltages.shape
    both = 2 * ports
    count = freq_index.shape[0]
    outer = times // INNER
    half = INNER // 2
    steps = count // (2 * COLUMNS)
    table = pltpu.VMEM((half, COLUMNS), jnp.bfloat16)
    turn = pltpu.VMEM((2 * outer, COLUMNS), jnp.float32)
    lines = in_hbm(freq_index.reshape(1, count))
    return pl.pallas_call(
        functools.partial(transform_body, inner=INNER, total=total),
        grid=(steps,),
        in_specs=[
            SMEM,
            SMEM,
            pl.BlockSpec((1, 2 * COLUMNS), lambda i: (0, i)),
            pl.BlockSpec((1, 2 * COLUMNS), lambda i: (0, jnp.minimum(i + 1, steps - 1))),
            HBM,
            HBM,
        ],
        out_specs=pl.BlockSpec((2 * COLUMNS // LANES, 2 * both, LANES), lambda i: (i, 0, 0)),
        out_shape=pltpu.VMEM((count // LANES, 2 * both, LANES), jnp.float32),
        scratch_shapes=[
            pltpu.VMEM((outer * both, half), jnp.bfloat16),
            pltpu.VMEM((outer * both, half), jnp.bfloat16),
            pltpu.VMEM((outer * both, INNER), jnp.bfloat16),
            table,
            table,
            table,
            table,
            turn,
            turn,
            pltpu.VMEM((ports, times), jnp.float32),
            pltpu.VMEM((ports, times), jnp.float32),
            pltpu.SemaphoreType.DMA((2, outer)),
        ],
        compiler_params=pltpu.CompilerParams(
            dimension_semantics=("arbitrary",), vmem_limit_bytes=48 << 20
        ),
        name="spectrum",
    )(first.reshape(1), in_hbm(start), lines, lines, in_hbm(voltages), in_hbm(currents))


def waves_body(impedance_ref, parts_ref, sent_ref, own_ref, share_ref, *, scale):
    ports = own_ref.shape[0]
    total = jnp.sum(parts_ref[...], axis=0) * scale
    z = as_column(impedance_ref, ports, jnp.float32)
    inverse = 1.0 / (2.0 * jnp.sqrt(z))
    power = jnp.zeros((ports, LANES), jnp.float32)
    for r in range(2):
        at = slice(r * LANES, (r + 1) * LANES)
        v = total[2 * r * ports : (2 * r + 1) * ports]
        c = total[(2 * r + 1) * ports : (2 * r + 2) * ports]
        a = (v + z * c) * inverse
        power = power + a * a
        sent_ref[:, at] = a
        own_ref[:, at] = (v - z * c) * inverse
    padded = jnp.concatenate([power, jnp.zeros((LANES - ports, LANES), jnp.float32)], axis=0)
    share = jnp.sum(padded.T, axis=0, keepdims=True)
    share_ref[...] = jnp.broadcast_to(share, share_ref.shape)


def means_body(shares_ref, out_ref, *, ports, width):
    row = lax.broadcasted_iota(jnp.int32, shares_ref.shape, 0)
    shares = shares_ref[...]
    lane = lax.broadcasted_iota(jnp.int32, (1, LANES), 1)
    sums = [
        jnp.sum(jnp.where((row & 1) == c, shares, 0.0), axis=0, keepdims=True) for c in range(2)
    ]
    both = jnp.where(lane < ports, sums[0], pltpu.roll(sums[1], ports, 1))
    out_ref[...] = jnp.broadcast_to(both / width + 1e-06, out_ref.shape)


def scatter_body(
    place_ref, pairing_ref, same_ref, other_ref, mean_0, mean_1, mean_2, mean_3,
    own_ref, out_ref, every_ref, table_ref, q_ref, mean_ref,
):
    ports = own_ref.shape[0]
    means = (mean_0, mean_1, mean_2, mean_3)
    place = place_ref[0]
    chips = len(means)
    every_ref[0] = same_ref[...]
    every_ref[1] = other_ref[...]
    lane = lax.broadcasted_iota(jnp.int32, (1, LANES), 1)
    for k in range(0, chips, 2):
        row = jnp.where(lane < 2 * ports, means[k][:1], pltpu.roll(means[k + 1][:1], 2 * ports, 1))
        table_ref[k * 2 * ports : (k + 2) * 2 * ports] = jnp.broadcast_to(row, (LANES, LANES)).T
    for p in range(ports):
        q = pairing_ref[p]
        holder = q // ports
        back = (place // 2 - holder // 2) & (chips - 1)
        rest = q % ports
        q_ref[p : p + 1] = every_ref[(place ^ holder) & 1, back, pl.ds(rest, 1)]
        mean_ref[p : p + 1] = table_ref[pl.ds((2 * back + (holder & 1)) * ports + rest, 1)]
    q_re, q_im = q_ref[:, :LANES], q_ref[:, LANES:]
    b_re, b_im = own_ref[:, :LANES], own_ref[:, LANES:]
    power = q_re * q_re + q_im * q_im
    inverse = 1.0 / jnp.maximum(power, 0.1 * mean_ref[...])
    out_ref[0] = (b_re * q_re + b_im * q_im) * inverse
    out_ref[1] = (b_im * q_re - b_re * q_im) * inverse


def body(voltages, currents, impedance, freq_index, window_start, pairing):
    ports, times = voltages.shape
    width = freq_index.shape[0]
    times_count, ports_count = lax.axis_size("tm"), lax.axis_size("port")
    chips = ports_count // 2
    total = times * times_count
    first = lax.axis_index("tm") * times
    parts = transform(first, window_start, freq_index, voltages, currents, total)
    parts = lax.all_to_all(in_vmem(parts), "tm", 0, 0, tiled=True)
    sent, own, share = pl.pallas_call(
        functools.partial(waves_body, scale=1.0 / math.sqrt(total)),
        in_specs=[SMEM, VMEM],
        out_specs=[VMEM, VMEM, VMEM],
        out_shape=[
            pltpu.VMEM((ports, 2 * LANES), jnp.float32),
            pltpu.VMEM((ports, 2 * LANES), jnp.float32),
            pltpu.VMEM((2 * times_count, LANES), jnp.float32),
        ],
        name="waves",
    )(in_hbm(impedance), in_vmem(parts))
    columns = [
        [ports_count * t + 2 * x + c for t in range(times_count) for c in range(2)]
        for x in range(chips)
    ]
    ahead = [
        [(i, (i + 2 * k) % ports_count) for i in range(ports_count)] for k in range(1, chips)
    ]
    shares = lax.all_to_all(
        in_vmem(share), ("tm", "port"), 0, 0, tiled=True, axis_index_groups=columns
    )
    along = [sent]
    for k in range(1, chips):
        along.append(lax.ppermute(sent, "port", ahead[k - 1]))
    same = jnp.stack(along)
    other = lax.ppermute(same, "port", [(i, i ^ 1) for i in range(ports_count)])
    mean = pl.pallas_call(
        functools.partial(means_body, ports=ports, width=width),
        in_specs=[VMEM],
        out_specs=VMEM,
        out_shape=pltpu.VMEM((8, LANES), jnp.float32),
        name="means",
    )(in_vmem(shares))
    means = [mean]
    for k in range(1, chips):
        means.append(lax.ppermute(mean, "port", ahead[k - 1]))
    return pl.pallas_call(
        scatter_body,
        in_specs=[SMEM, SMEM] + [VMEM] * (chips + 3),
        out_specs=VMEM,
        out_shape=jax.ShapeDtypeStruct((2, ports, LANES), jnp.float32),
        scratch_shapes=[
            pltpu.VMEM((2, chips, ports, 2 * LANES), jnp.float32),
            pltpu.VMEM((ports_count * ports, LANES), jnp.float32),
            pltpu.VMEM((ports, 2 * LANES), jnp.float32),
            pltpu.VMEM((ports, LANES), jnp.float32),
        ],
        name="scatter",
    )(
        lax.axis_index("port").reshape(1), in_hbm(pairing), in_vmem(same), in_vmem(other),
        *map(in_vmem, means), in_vmem(own),
    )


def solution(mesh):
    placed = (P("port", "tm"), P("port", "tm"), P("port"), P(), P("port"), P("port"))
    return jax.shard_map(
        body, mesh=mesh, in_specs=placed, out_specs=P(None, "port", "tm"), check_vma=False
    )
```

```python
import functools
import math

import jax
import jax.numpy as jnp
from jax import lax
from jax.experimental import pallas as pl
from jax.experimental.pallas import tpu as pltpu
from jax.sharding import PartitionSpec as P


LANES = 128
COLUMNS = 256
INNER = 1024
FLIP = 256
VMEM = pl.BlockSpec(memory_space=pltpu.VMEM)
HBM = pl.BlockSpec(memory_space=pltpu.HBM)


def in_hbm(array):
    return pltpu.with_memory_space_constraint(array, pltpu.HBM)


def in_vmem(array):
    return pltpu.with_memory_space_constraint(array, pltpu.VMEM)


def turned(phase, total):
    bits = total.bit_length() - 1
    wrapped = phase & (total - 1)
    quarter = (wrapped + total // 8) >> (bits - 2)
    rest = wrapped - (quarter << (bits - 2))
    x = rest.astype(jnp.float32) * (2.0 * math.pi / total)
    y = x * x
    sine = x + x * y * (-1.6666654611e-1 + y * (8.3321608736e-3 - y * 1.9515295891e-4))
    cosine = (
        1.0
        - 0.5 * y
        + y * y * (4.166664568298827e-2 + y * (-1.388731625493765e-3 + y * 2.443315711809948e-5))
    )
    odd = (quarter & 1) == 1
    even_part = jnp.where(odd, sine, cosine)
    odd_part = jnp.where(odd, cosine, sine)
    flip = ((quarter + 1) & 2) == 2
    below = (quarter & 2) == 2
    return jnp.where(flip, -even_part, even_part), jnp.where(below, odd_part, -odd_part)


def as_column(scalars, rows, dtype):
    row = lax.broadcasted_iota(jnp.int32, (rows, LANES), 0)
    column = jnp.zeros((rows, LANES), dtype)
    for r in range(rows):
        column = jnp.where(row == r, scalars[r], column)
    return column


def transform_body(
    start_ref, impedance_ref, pairing_ref, lines_ref, v_ref, c_ref, out_ref, z_ref, driven_ref,
    even_ref, odd_ref, raw_ref, cos_0, sin_0, cos_1, sin_1, turn_0, turn_1, v_in, c_in, lines_in,
    start_in, impedance_in, pairing_in, sems, small_sems,
    *, inner, total
):
    ports, times = v_ref.shape
    both = 2 * ports
    outer = times // inner
    half = inner // 2
    cols = COLUMNS
    first = lax.axis_index("tm") * times
    step, steps_count = pl.program_id(0), pl.num_programs(0)

    def lines_of(tile):
        return lines_in[:, pl.ds(pl.multiple_of(tile * cols, cols), cols)]

    small = [
        pltpu.make_async_copy(a, b, small_sems.at[n])
        for n, (a, b) in enumerate(
            (
                (lines_ref, lines_in),
                (start_ref, start_in),
                (impedance_ref, impedance_in),
                (pairing_ref, pairing_in),
            )
        )
    ]

    def copies(s):
        at = pl.ds(s * inner, inner)
        return (
            pltpu.make_async_copy(v_ref.at[:, at], v_in.at[:, at], sems.at[0, s]),
            pltpu.make_async_copy(c_ref.at[:, at], c_in.at[:, at], sems.at[1, s]),
        )

    def build(lines, cos_ref, sin_ref, turn_ref):
        def steps(count):
            return lax.broadcasted_iota(jnp.int32, (count, cols), 0)

        fine = 16
        coarse = half // fine
        fine_cos, fine_sin = turned(lines * (2 * steps(fine) + 1), 2 * total)
        coarse_cos, coarse_sin = turned(lines * (steps(coarse) * (2 * fine)), 2 * total)
        middle = 2 * (first + steps(outer) * inner + half) - 1
        turn_ref[:outer], turn_ref[outer:] = turned(lines * middle, 2 * total)
        for u in range(coarse):
            cos_u, sin_u = coarse_cos[u : u + 1], coarse_sin[u : u + 1]
            at = slice(u * fine, (u + 1) * fine)
            cos_ref[at] = (cos_u * fine_cos - sin_u * fine_sin).astype(jnp.bfloat16)
            sin_ref[at] = (sin_u * fine_cos + cos_u * fine_sin).astype(jnp.bfloat16)

    def spectra(cos_ref, sin_ref, turn_ref, base):
        group = max(1, 512 // both)
        re = jnp.zeros((both, cols), jnp.float32)
        im = jnp.zeros((both, cols), jnp.float32)
        for g in range(0, outer, group):
            at = slice(g * both, (g + group) * both)
            part_re = jnp.dot(even_ref[at], cos_ref[...], preferred_element_type=jnp.float32)
            part_im = jnp.dot(odd_ref[at], sin_ref[...], preferred_element_type=jnp.float32)
            for s in range(group):
                re_s = part_re[s * both : (s + 1) * both]
                im_s = part_im[s * both : (s + 1) * both]
                cos_s = turn_ref[g + s : g + s + 1]
                sin_s = turn_ref[outer + g + s : outer + g + s + 1]
                re = re + (re_s * cos_s - im_s * sin_s)
                im = im + (re_s * sin_s + im_s * cos_s)
        for j in range(cols // LANES):
            at = slice(j * LANES, (j + 1) * LANES)
            out_ref[base + j, :both] = re[:, at]
            out_ref[base + j, both:] = im[:, at]

    @pl.when(step == 0)
    def _():
        small[0].start()
        for s in range(outer):
            for copy in copies(s):
                copy.start()
        for copy in small[1:]:
            copy.start()
        small[0].wait()
        build(lines_of(0), cos_0, sin_0, turn_0)
        for copy in small[1:]:
            copy.wait()
        start = as_column(start_in, ports, jnp.int32)[:, :1]
        z_ref[...] = as_column(impedance_in, ports, jnp.float32)
        driven_ref[...] = as_column(pairing_in, ports, jnp.int32)
        row = lax.broadcasted_iota(jnp.int32, (FLIP, FLIP), 0)
        col = lax.broadcasted_iota(jnp.int32, (FLIP, FLIP), 1)
        flip = jnp.where(row + col == FLIP - 1, 1.0, 0.0).astype(jnp.bfloat16)
        group = max(1, 256 // both)
        for g in range(0, outer, group):
            for s in range(g, g + group):
                at = slice(s * inner, (s + 1) * inner)
                time = first + s * inner
                time = time + lax.broadcasted_iota(jnp.int32, (ports, inner), 1)
                keep = time >= start
                low = s * both
                for copy in copies(s):
                    copy.wait()
                raw_ref[low : low + ports] = jnp.where(keep, v_in[:, at], 0.0).astype(jnp.bfloat16)
                raw_ref[low + ports : low + both] = jnp.where(keep, c_in[:, at], 0.0).astype(
                    jnp.bfloat16
                )
            at = slice(g * both, (g + group) * both)
            for q in range(half // FLIP):
                to = slice(q * FLIP, (q + 1) * FLIP)
                behind = jnp.dot(
                    raw_ref[at, half - (q + 1) * FLIP : half - q * FLIP],
                    flip,
                    preferred_element_type=jnp.float32,
                )
                ahead = raw_ref[at, half + q * FLIP : half + (q + 1) * FLIP].astype(jnp.float32)
                even_ref[at, to] = (ahead + behind).astype(jnp.bfloat16)
                odd_ref[at, to] = (ahead - behind).astype(jnp.bfloat16)

    build(lines_of(2 * step + 1), cos_1, sin_1, turn_1)
    spectra(cos_0, sin_0, turn_0, 0)
    build(lines_of(2 * jnp.minimum(step + 1, steps_count - 1)), cos_0, sin_0, turn_0)
    spectra(cos_1, sin_1, turn_1, cols // LANES)


def transform(start, impedance, pairing, freq_index, voltages, currents, total):
    ports, times = voltages.shape
    both = 2 * ports
    count = freq_index.shape[0]
    outer = times // INNER
    half = INNER // 2
    table = pltpu.VMEM((half, COLUMNS), jnp.bfloat16)
    turn = pltpu.VMEM((2 * outer, COLUMNS), jnp.float32)
    column = pl.BlockSpec((ports, LANES), lambda i: (0, 0))
    return pl.pallas_call(
        functools.partial(transform_body, inner=INNER, total=total),
        grid=(count // (2 * COLUMNS),),
        in_specs=[HBM] * 6,
        out_specs=[
            pl.BlockSpec((2 * COLUMNS // LANES, 2 * both, LANES), lambda i: (i, 0, 0)),
            column,
            column,
        ],
        out_shape=[
            pltpu.VMEM((count // LANES, 2 * both, LANES), jnp.float32),
            pltpu.VMEM((ports, LANES), jnp.float32),
            pltpu.VMEM((ports, LANES), jnp.int32),
        ],
        scratch_shapes=[
            pltpu.VMEM((outer * both, half), jnp.bfloat16),
            pltpu.VMEM((outer * both, half), jnp.bfloat16),
            pltpu.VMEM((outer * both, INNER), jnp.bfloat16),
            table,
            table,
            table,
            table,
            turn,
            turn,
            pltpu.VMEM((ports, times), jnp.float32),
            pltpu.VMEM((ports, times), jnp.float32),
            pltpu.VMEM((1, count), jnp.int32),
            pltpu.SMEM((ports,), jnp.int32),
            pltpu.SMEM((ports,), jnp.float32),
            pltpu.SMEM((ports,), jnp.int32),
            pltpu.SemaphoreType.DMA((2, outer)),
            pltpu.SemaphoreType.DMA((4,)),
        ],
        compiler_params=pltpu.CompilerParams(
            dimension_semantics=("arbitrary",), vmem_limit_bytes=48 << 20
        ),
        name="spectrum",
    )(
        in_hbm(start), in_hbm(impedance), in_hbm(pairing), in_hbm(freq_index.reshape(1, count)),
        in_hbm(voltages), in_hbm(currents),
    )


def waves_body(z_ref, parts_ref, sent_ref, own_ref, share_ref, *, scale):
    ports = own_ref.shape[0]
    total = jnp.sum(parts_ref[...], axis=0) * scale
    z = z_ref[...]
    inverse = 1.0 / (2.0 * jnp.sqrt(z))
    power = jnp.zeros((ports, LANES), jnp.float32)
    for r in range(2):
        at = slice(r * LANES, (r + 1) * LANES)
        v = total[2 * r * ports : (2 * r + 1) * ports]
        c = total[(2 * r + 1) * ports : (2 * r + 2) * ports]
        a = (v + z * c) * inverse
        power = power + a * a
        sent_ref[:, at] = a
        own_ref[:, at] = (v - z * c) * inverse
    padded = jnp.concatenate([power, jnp.zeros((LANES - ports, LANES), jnp.float32)], axis=0)
    share = jnp.sum(padded.T, axis=0, keepdims=True)
    share_ref[...] = jnp.broadcast_to(share, share_ref.shape)


def means_body(shares_ref, out_ref, *, ports, width):
    row = lax.broadcasted_iota(jnp.int32, shares_ref.shape, 0)
    shares = shares_ref[...]
    lane = lax.broadcasted_iota(jnp.int32, (1, LANES), 1)
    sums = [
        jnp.sum(jnp.where((row & 1) == c, shares, 0.0), axis=0, keepdims=True) for c in range(2)
    ]
    both = jnp.where(lane < ports, sums[0], pltpu.roll(sums[1], ports, 1))
    out_ref[...] = jnp.broadcast_to(both / width + 1e-06, out_ref.shape)


def scatter_body(driven_ref, same_ref, other_ref, mean_0, mean_1, mean_2, mean_3, own_ref, out_ref):
    ports = own_ref.shape[0]
    means = (mean_0, mean_1, mean_2, mean_3)
    chips = len(means)
    place = lax.axis_index("port")
    driven = driven_ref[...]
    holder = driven // ports
    rest = driven % ports
    back = (place // 2 - holder // 2) & (chips - 1)
    core = holder & 1
    lane = lax.broadcasted_iota(jnp.int32, (ports, LANES), 1)
    spot = back * ports + rest
    q = jnp.zeros((ports, 2 * LANES), jnp.float32)
    for swapped, held_ref in enumerate((same_ref, other_ref)):
        here = (lane == spot) & (((place + core) & 1) == swapped)
        picks = jnp.where(here, 1.0, 0.0).astype(jnp.bfloat16)
        left = held_ref[...].reshape(chips * ports, 2 * LANES)
        for _ in range(3):
            term = left.astype(jnp.bfloat16)
            q = q + jnp.dot(picks, term, preferred_element_type=jnp.float32)
            left = left - term.astype(jnp.float32)
    level = jnp.zeros((ports, LANES), jnp.float32)
    for k in range(chips):
        here = (lane == core * ports + rest) & (back == k)
        level = level + jnp.where(here, means[k][:1], 0.0)
    mean = jnp.sum(level, axis=1, keepdims=True)
    q_re, q_im = q[:, :LANES], q[:, LANES:]
    b_re, b_im = own_ref[:, :LANES], own_ref[:, LANES:]
    power = q_re * q_re + q_im * q_im
    inverse = 1.0 / jnp.maximum(power, 0.1 * mean)
    out_ref[0] = (b_re * q_re + b_im * q_im) * inverse
    out_ref[1] = (b_im * q_re - b_re * q_im) * inverse


def body(voltages, currents, impedance, freq_index, window_start, pairing):
    ports, times = voltages.shape
    width = freq_index.shape[0]
    times_count, ports_count = lax.axis_size("tm"), lax.axis_size("port")
    chips = ports_count // 2
    total = times * times_count
    parts, z, driven = transform(
        window_start, impedance, pairing, freq_index, voltages, currents, total
    )
    parts = lax.all_to_all(in_vmem(parts), "tm", 0, 0, tiled=True)
    sent, own, share = pl.pallas_call(
        functools.partial(waves_body, scale=1.0 / math.sqrt(total)),
        in_specs=[VMEM, VMEM],
        out_specs=[VMEM, VMEM, VMEM],
        out_shape=[
            pltpu.VMEM((ports, 2 * LANES), jnp.float32),
            pltpu.VMEM((ports, 2 * LANES), jnp.float32),
            pltpu.VMEM((2 * times_count, LANES), jnp.float32),
        ],
        name="waves",
    )(in_vmem(z), in_vmem(parts))
    columns = [
        [ports_count * t + 2 * x + c for t in range(times_count) for c in range(2)]
        for x in range(chips)
    ]
    ahead = [
        [(i, (i + 2 * k) % ports_count) for i in range(ports_count)] for k in range(1, chips)
    ]
    shares = lax.all_to_all(
        in_vmem(share), ("tm", "port"), 0, 0, tiled=True, axis_index_groups=columns
    )
    along = [sent]
    for k in range(1, chips):
        along.append(lax.ppermute(sent, "port", ahead[k - 1]))
    same = jnp.stack(along)
    other = lax.ppermute(same, "port", [(i, i ^ 1) for i in range(ports_count)])
    mean = pl.pallas_call(
        functools.partial(means_body, ports=ports, width=width),
        in_specs=[VMEM],
        out_specs=VMEM,
        out_shape=pltpu.VMEM((8, LANES), jnp.float32),
        name="means",
    )(in_vmem(shares))
    means = [mean]
    for k in range(1, chips):
        means.append(lax.ppermute(mean, "port", ahead[k - 1]))
    return pl.pallas_call(
        scatter_body,
        in_specs=[VMEM] * (chips + 4),
        out_specs=VMEM,
        out_shape=jax.ShapeDtypeStruct((2, ports, LANES), jnp.float32),
        name="scatter",
    )(
        in_vmem(driven), in_vmem(same), in_vmem(other), *map(in_vmem, means), in_vmem(own),
    )


def solution(mesh):
    placed = (P("port", "tm"), P("port", "tm"), P("port"), P(), P("port"), P("port"))
    return jax.shard_map(
        body, mesh=mesh, in_specs=placed, out_specs=P(None, "port", "tm"), check_vma=False
    )
```

```python
import functools
import math

import jax
import jax.numpy as jnp
from jax import lax
from jax.experimental import pallas as pl
from jax.experimental.pallas import tpu as pltpu
from jax.sharding import PartitionSpec as P


LANES = 128
COLUMNS = 256
INNER = 1024
FLIP = 256
BLOCK = 16
VMEM = pl.BlockSpec(memory_space=pltpu.VMEM)
HBM = pl.BlockSpec(memory_space=pltpu.HBM)


def in_hbm(array):
    return pltpu.with_memory_space_constraint(array, pltpu.HBM)


def in_vmem(array):
    return pltpu.with_memory_space_constraint(array, pltpu.VMEM)


def turned(phase, total):
    bits = total.bit_length() - 1
    wrapped = phase & (total - 1)
    quarter = (wrapped + total // 8) >> (bits - 2)
    rest = wrapped - (quarter << (bits - 2))
    x = rest.astype(jnp.float32) * (2.0 * math.pi / total)
    y = x * x
    sine = x + x * y * (-1.6666654611e-1 + y * (8.3321608736e-3 - y * 1.9515295891e-4))
    cosine = (
        1.0
        - 0.5 * y
        + y * y * (4.166664568298827e-2 + y * (-1.388731625493765e-3 + y * 2.443315711809948e-5))
    )
    odd = (quarter & 1) == 1
    even_part = jnp.where(odd, sine, cosine)
    odd_part = jnp.where(odd, cosine, sine)
    flip = ((quarter + 1) & 2) == 2
    below = (quarter & 2) == 2
    return jnp.where(flip, -even_part, even_part), jnp.where(below, odd_part, -odd_part)


def as_column(scalars, rows, dtype):
    row = lax.broadcasted_iota(jnp.int32, (rows, LANES), 0)
    column = jnp.zeros((rows, LANES), dtype)
    for r in range(rows):
        column = jnp.where(row == r, scalars[r], column)
    return column


def transform_body(
    start_ref, impedance_ref, pairing_ref, lines_ref, v_ref, c_ref, out_ref, z_ref, driven_ref,
    even_ref, odd_ref, raw_ref, cos_0, sin_0, cos_1, sin_1, turn_0, turn_1, v_in, c_in, lines_in,
    start_in, impedance_in, pairing_in, sems, small_sems,
    *, inner, total
):
    ports, times = v_ref.shape
    both = 2 * ports
    outer = times // inner
    half = inner // 2
    cols = COLUMNS
    first = lax.axis_index("tm") * times
    step, steps_count = pl.program_id(0), pl.num_programs(0)

    def lines_of(tile):
        return lines_in[:, pl.ds(pl.multiple_of(tile * cols, cols), cols)]

    small = [
        pltpu.make_async_copy(a, b, small_sems.at[n])
        for n, (a, b) in enumerate(
            (
                (lines_ref, lines_in),
                (start_ref, start_in),
                (impedance_ref, impedance_in),
                (pairing_ref, pairing_in),
            )
        )
    ]

    def copies(s):
        at = pl.ds(s * inner, inner)
        return (
            pltpu.make_async_copy(v_ref.at[:, at], v_in.at[:, at], sems.at[0, s]),
            pltpu.make_async_copy(c_ref.at[:, at], c_in.at[:, at], sems.at[1, s]),
        )

    def build(lines, cos_ref, sin_ref, turn_ref):
        def steps(count):
            return lax.broadcasted_iota(jnp.int32, (count, cols), 0)

        fine = 16
        coarse = half // fine
        fine_cos, fine_sin = turned(lines * (2 * steps(fine) + 1), 2 * total)
        coarse_cos, coarse_sin = turned(lines * (steps(coarse) * (2 * fine)), 2 * total)
        middle = 2 * (first + steps(outer) * inner + half) - 1
        turn_ref[:outer], turn_ref[outer:] = turned(lines * middle, 2 * total)
        for u in range(coarse):
            cos_u, sin_u = coarse_cos[u : u + 1], coarse_sin[u : u + 1]
            at = slice(u * fine, (u + 1) * fine)
            cos_ref[at] = (cos_u * fine_cos - sin_u * fine_sin).astype(jnp.bfloat16)
            sin_ref[at] = (sin_u * fine_cos + cos_u * fine_sin).astype(jnp.bfloat16)

    def spectra(cos_ref, sin_ref, turn_ref, base):
        deep = outer * BLOCK
        group = max(1, 1024 // deep)
        for g in range(0, both // BLOCK, group):
            at = slice(g * deep, (g + group) * deep)
            part_re = jnp.dot(even_ref[at], cos_ref[...], preferred_element_type=jnp.float32)
            part_im = jnp.dot(odd_ref[at], sin_ref[...], preferred_element_type=jnp.float32)
            for b in range(group):
                re = jnp.zeros((BLOCK, cols), jnp.float32)
                im = jnp.zeros((BLOCK, cols), jnp.float32)
                for s in range(outer):
                    low = b * deep + s * BLOCK
                    re_s = part_re[low : low + BLOCK]
                    im_s = part_im[low : low + BLOCK]
                    cos_s = turn_ref[s : s + 1]
                    sin_s = turn_ref[outer + s : outer + s + 1]
                    re = re + (re_s * cos_s - im_s * sin_s)
                    im = im + (re_s * sin_s + im_s * cos_s)
                low = (g + b) * BLOCK
                for j in range(cols // LANES):
                    at = slice(j * LANES, (j + 1) * LANES)
                    out_ref[base + j, low : low + BLOCK] = re[:, at]
                    out_ref[base + j, both + low : both + low + BLOCK] = im[:, at]

    @pl.when(step == 0)
    def _():
        small[0].start()
        for s in range(outer):
            for copy in copies(s):
                copy.start(priority=1)
        for copy in small[1:]:
            copy.start()
        small[0].wait()
        build(lines_of(0), cos_0, sin_0, turn_0)
        for copy in small[1:]:
            copy.wait()
        start = as_column(start_in, ports, jnp.int32)[:, :1]
        z_ref[...] = as_column(impedance_in, ports, jnp.float32)
        driven_ref[...] = as_column(pairing_in, ports, jnp.int32)
        row = lax.broadcasted_iota(jnp.int32, (FLIP, FLIP), 0)
        col = lax.broadcasted_iota(jnp.int32, (FLIP, FLIP), 1)
        flip = jnp.where(row + col == FLIP - 1, 1.0, 0.0).astype(jnp.bfloat16)
        deep = outer * BLOCK
        group = max(1, 512 // both)
        for g in range(0, outer, group):
            for s in range(g, g + group):
                at = slice(s * inner, (s + 1) * inner)
                time = first + s * inner
                time = time + lax.broadcasted_iota(jnp.int32, (ports, inner), 1)
                keep = time >= start
                for copy in copies(s):
                    copy.wait()
                gated_v = jnp.where(keep, v_in[:, at], 0.0).astype(jnp.bfloat16)
                gated_c = jnp.where(keep, c_in[:, at], 0.0).astype(jnp.bfloat16)
                for b in range(ports // BLOCK):
                    of = slice(b * BLOCK, (b + 1) * BLOCK)
                    low = b * deep + s * BLOCK
                    raw_ref[low : low + BLOCK] = gated_v[of]
                    low += ports // BLOCK * deep
                    raw_ref[low : low + BLOCK] = gated_c[of]
            for b in range(both // BLOCK):
                at = slice(b * deep + g * BLOCK, b * deep + (g + group) * BLOCK)
                for q in range(half // FLIP):
                    to = slice(q * FLIP, (q + 1) * FLIP)
                    behind = jnp.dot(
                        raw_ref[at, half - (q + 1) * FLIP : half - q * FLIP],
                        flip,
                        preferred_element_type=jnp.float32,
                    )
                    ahead = raw_ref[at, half + q * FLIP : half + (q + 1) * FLIP]
                    ahead = ahead.astype(jnp.float32)
                    even_ref[at, to] = (ahead + behind).astype(jnp.bfloat16)
                    odd_ref[at, to] = (ahead - behind).astype(jnp.bfloat16)

    build(lines_of(2 * step + 1), cos_1, sin_1, turn_1)
    spectra(cos_0, sin_0, turn_0, 0)
    build(lines_of(2 * jnp.minimum(step + 1, steps_count - 1)), cos_0, sin_0, turn_0)
    spectra(cos_1, sin_1, turn_1, cols // LANES)


def transform(start, impedance, pairing, freq_index, voltages, currents, total):
    ports, times = voltages.shape
    both = 2 * ports
    count = freq_index.shape[0]
    outer = times // INNER
    half = INNER // 2
    table = pltpu.VMEM((half, COLUMNS), jnp.bfloat16)
    turn = pltpu.VMEM((2 * outer, COLUMNS), jnp.float32)
    column = pl.BlockSpec((ports, LANES), lambda i: (0, 0))
    return pl.pallas_call(
        functools.partial(transform_body, inner=INNER, total=total),
        grid=(count // (2 * COLUMNS),),
        in_specs=[HBM] * 6,
        out_specs=[
            pl.BlockSpec((2 * COLUMNS // LANES, 2 * both, LANES), lambda i: (i, 0, 0)),
            column,
            column,
        ],
        out_shape=[
            pltpu.VMEM((count // LANES, 2 * both, LANES), jnp.float32),
            pltpu.VMEM((ports, LANES), jnp.float32),
            pltpu.VMEM((ports, LANES), jnp.int32),
        ],
        scratch_shapes=[
            pltpu.VMEM((outer * both, half), jnp.bfloat16),
            pltpu.VMEM((outer * both, half), jnp.bfloat16),
            pltpu.VMEM((outer * both, INNER), jnp.bfloat16),
            table,
            table,
            table,
            table,
            turn,
            turn,
            pltpu.VMEM((ports, times), jnp.float32),
            pltpu.VMEM((ports, times), jnp.float32),
            pltpu.VMEM((1, count), jnp.int32),
            pltpu.SMEM((ports,), jnp.int32),
            pltpu.SMEM((ports,), jnp.float32),
            pltpu.SMEM((ports,), jnp.int32),
            pltpu.SemaphoreType.DMA((2, outer)),
            pltpu.SemaphoreType.DMA((4,)),
        ],
        compiler_params=pltpu.CompilerParams(
            dimension_semantics=("arbitrary",), vmem_limit_bytes=48 << 20
        ),
        name="spectrum",
    )(
        in_hbm(start), in_hbm(impedance), in_hbm(pairing), in_hbm(freq_index.reshape(1, count)),
        in_hbm(voltages), in_hbm(currents),
    )


def waves_body(z_ref, parts_ref, sent_ref, own_ref, share_ref, *, scale):
    ports = own_ref.shape[0]
    total = jnp.sum(parts_ref[...], axis=0) * scale
    z = z_ref[...]
    inverse = 1.0 / (2.0 * jnp.sqrt(z))
    power = jnp.zeros((ports, LANES), jnp.float32)
    for r in range(2):
        at = slice(r * LANES, (r + 1) * LANES)
        v = total[2 * r * ports : (2 * r + 1) * ports]
        c = total[(2 * r + 1) * ports : (2 * r + 2) * ports]
        a = (v + z * c) * inverse
        power = power + a * a
        sent_ref[:, at] = a
        own_ref[:, at] = (v - z * c) * inverse
    padded = jnp.concatenate([power, jnp.zeros((LANES - ports, LANES), jnp.float32)], axis=0)
    share = jnp.sum(padded.T, axis=0, keepdims=True)
    share_ref[...] = jnp.broadcast_to(share, share_ref.shape)


def means_body(shares_ref, out_ref, *, ports, width):
    row = lax.broadcasted_iota(jnp.int32, shares_ref.shape, 0)
    shares = shares_ref[...]
    lane = lax.broadcasted_iota(jnp.int32, (1, LANES), 1)
    sums = [
        jnp.sum(jnp.where((row & 1) == c, shares, 0.0), axis=0, keepdims=True) for c in range(2)
    ]
    both = jnp.where(lane < ports, sums[0], pltpu.roll(sums[1], ports, 1))
    out_ref[...] = jnp.broadcast_to(both / width + 1e-06, out_ref.shape)


def scatter_body(driven_ref, same_ref, other_ref, mean_0, mean_1, mean_2, mean_3, own_ref, out_ref):
    ports = own_ref.shape[0]
    means = (mean_0, mean_1, mean_2, mean_3)
    chips = len(means)
    place = lax.axis_index("port")
    driven = driven_ref[...]
    holder = driven // ports
    rest = driven % ports
    back = (place // 2 - holder // 2) & (chips - 1)
    core = holder & 1
    lane = lax.broadcasted_iota(jnp.int32, (ports, LANES), 1)
    spot = back * ports + rest
    q = jnp.zeros((ports, 2 * LANES), jnp.float32)
    for swapped, held_ref in enumerate((same_ref, other_ref)):
        here = (lane == spot) & (((place + core) & 1) == swapped)
        picks = jnp.where(here, 1.0, 0.0).astype(jnp.bfloat16)
        left = held_ref[...].reshape(chips * ports, 2 * LANES)
        for _ in range(3):
            term = left.astype(jnp.bfloat16)
            q = q + jnp.dot(picks, term, preferred_element_type=jnp.float32)
            left = left - term.astype(jnp.float32)
    level = jnp.zeros((ports, LANES), jnp.float32)
    for k in range(chips):
        here = (lane == core * ports + rest) & (back == k)
        level = level + jnp.where(here, means[k][:1], 0.0)
    mean = jnp.sum(level, axis=1, keepdims=True)
    q_re, q_im = q[:, :LANES], q[:, LANES:]
    b_re, b_im = own_ref[:, :LANES], own_ref[:, LANES:]
    power = q_re * q_re + q_im * q_im
    inverse = 1.0 / jnp.maximum(power, 0.1 * mean)
    out_ref[0] = (b_re * q_re + b_im * q_im) * inverse
    out_ref[1] = (b_im * q_re - b_re * q_im) * inverse


def body(voltages, currents, impedance, freq_index, window_start, pairing):
    ports, times = voltages.shape
    width = freq_index.shape[0]
    times_count, ports_count = lax.axis_size("tm"), lax.axis_size("port")
    chips = ports_count // 2
    total = times * times_count
    parts, z, driven = transform(
        window_start, impedance, pairing, freq_index, voltages, currents, total
    )
    parts = lax.all_to_all(in_vmem(parts), "tm", 0, 0, tiled=True)
    sent, own, share = pl.pallas_call(
        functools.partial(waves_body, scale=1.0 / math.sqrt(total)),
        in_specs=[VMEM, VMEM],
        out_specs=[VMEM, VMEM, VMEM],
        out_shape=[
            pltpu.VMEM((ports, 2 * LANES), jnp.float32),
            pltpu.VMEM((ports, 2 * LANES), jnp.float32),
            pltpu.VMEM((2 * times_count, LANES), jnp.float32),
        ],
        name="waves",
    )(in_vmem(z), in_vmem(parts))
    columns = [
        [ports_count * t + 2 * x + c for t in range(times_count) for c in range(2)]
        for x in range(chips)
    ]
    ahead = [
        [(i, (i + 2 * k) % ports_count) for i in range(ports_count)] for k in range(1, chips)
    ]
    shares = lax.all_to_all(
        in_vmem(share), ("tm", "port"), 0, 0, tiled=True, axis_index_groups=columns
    )
    along = [sent]
    for k in range(1, chips):
        along.append(lax.ppermute(sent, "port", ahead[k - 1]))
    same = jnp.stack(along)
    other = lax.ppermute(same, "port", [(i, i ^ 1) for i in range(ports_count)])
    mean = pl.pallas_call(
        functools.partial(means_body, ports=ports, width=width),
        in_specs=[VMEM],
        out_specs=VMEM,
        out_shape=pltpu.VMEM((8, LANES), jnp.float32),
        name="means",
    )(in_vmem(shares))
    means = [mean]
    for k in range(1, chips):
        means.append(lax.ppermute(mean, "port", ahead[k - 1]))
    return pl.pallas_call(
        scatter_body,
        in_specs=[VMEM] * (chips + 4),
        out_specs=VMEM,
        out_shape=jax.ShapeDtypeStruct((2, ports, LANES), jnp.float32),
        name="scatter",
    )(
        in_vmem(driven), in_vmem(same), in_vmem(other), *map(in_vmem, means), in_vmem(own),
    )


def solution(mesh):
    placed = (P("port", "tm"), P("port", "tm"), P("port"), P(), P("port"), P("port"))
    return jax.shard_map(
        body, mesh=mesh, in_specs=placed, out_specs=P(None, "port", "tm"), check_vma=False
    )
```

```python
import functools
import math

import jax
import jax.numpy as jnp
from jax import lax
from jax.experimental import pallas as pl
from jax.experimental.pallas import tpu as pltpu
from jax.sharding import PartitionSpec as P


LANES = 128
COLUMNS = 256
INNER = 1024
FLIP = 256
BLOCK = 16
VMEM = pl.BlockSpec(memory_space=pltpu.VMEM)
HBM = pl.BlockSpec(memory_space=pltpu.HBM)


def in_hbm(array):
    return pltpu.with_memory_space_constraint(array, pltpu.HBM)


def in_vmem(array):
    return pltpu.with_memory_space_constraint(array, pltpu.VMEM)


def turned(phase, total):
    bits = total.bit_length() - 1
    wrapped = phase & (total - 1)
    quarter = (wrapped + total // 8) >> (bits - 2)
    rest = wrapped - (quarter << (bits - 2))
    x = rest.astype(jnp.float32) * (2.0 * math.pi / total)
    y = x * x
    sine = x + x * y * (-1.6666654611e-1 + y * (8.3321608736e-3 - y * 1.9515295891e-4))
    cosine = (
        1.0
        - 0.5 * y
        + y * y * (4.166664568298827e-2 + y * (-1.388731625493765e-3 + y * 2.443315711809948e-5))
    )
    odd = (quarter & 1) == 1
    even_part = jnp.where(odd, sine, cosine)
    odd_part = jnp.where(odd, cosine, sine)
    flip = ((quarter + 1) & 2) == 2
    below = (quarter & 2) == 2
    return jnp.where(flip, -even_part, even_part), jnp.where(below, odd_part, -odd_part)


def as_column(scalars, rows, dtype):
    row = lax.broadcasted_iota(jnp.int32, (rows, LANES), 0)
    column = jnp.zeros((rows, LANES), dtype)
    for r in range(rows):
        column = jnp.where(row == r, scalars[r], column)
    return column


def transform_body(
    start_ref, impedance_ref, pairing_ref, lines_ref, v_ref, c_ref, out_ref, z_ref, driven_ref,
    even_ref, odd_ref, raw_ref, cos_0, sin_0, cos_1, sin_1, turn_0, turn_1, v_in, c_in, lines_in,
    start_in, impedance_in, pairing_in, sems, small_sems,
    *, inner, total
):
    ports, times = v_ref.shape
    both = 2 * ports
    outer = times // inner
    half = inner // 2
    cols = COLUMNS
    first = lax.axis_index("tm") * times
    step, steps_count = pl.program_id(0), pl.num_programs(0)

    def lines_of(tile):
        return lines_in[:, pl.ds(pl.multiple_of(tile * cols, cols), cols)]

    small = [
        pltpu.make_async_copy(a, b, small_sems.at[n])
        for n, (a, b) in enumerate(
            (
                (lines_ref, lines_in),
                (start_ref, start_in),
                (impedance_ref, impedance_in),
                (pairing_ref, pairing_in),
            )
        )
    ]

    def copies(s):
        at = pl.ds(s * inner, inner)
        return (
            pltpu.make_async_copy(v_ref.at[:, at], v_in.at[:, at], sems.at[0, s]),
            pltpu.make_async_copy(c_ref.at[:, at], c_in.at[:, at], sems.at[1, s]),
        )

    def build(lines, cos_ref, sin_ref, turn_ref):
        def steps(count):
            return lax.broadcasted_iota(jnp.int32, (count, cols), 0)

        fine = 16
        coarse = half // fine
        fine_cos, fine_sin = turned(lines * (2 * steps(fine) + 1), 2 * total)
        near_cos, near_sin = turned(lines * (steps(8) * (2 * fine)), 2 * total)
        far_cos, far_sin = turned(lines * (steps(coarse // 8) * (16 * fine)), 2 * total)
        coarse_cos, coarse_sin = [], []
        for u in range(coarse // 8):
            cos_u, sin_u = far_cos[u : u + 1], far_sin[u : u + 1]
            coarse_cos.append(cos_u * near_cos - sin_u * near_sin)
            coarse_sin.append(sin_u * near_cos + cos_u * near_sin)
        coarse_cos = jnp.concatenate(coarse_cos, axis=0)
        coarse_sin = jnp.concatenate(coarse_sin, axis=0)
        middle = 2 * (first + steps(outer) * inner + half) - 1
        turn_ref[:outer], turn_ref[outer:] = turned(lines * middle, 2 * total)
        for u in range(coarse):
            cos_u, sin_u = coarse_cos[u : u + 1], coarse_sin[u : u + 1]
            at = slice(u * fine, (u + 1) * fine)
            cos_ref[at] = (cos_u * fine_cos - sin_u * fine_sin).astype(jnp.bfloat16)
            sin_ref[at] = (sin_u * fine_cos + cos_u * fine_sin).astype(jnp.bfloat16)

    def spectra(cos_ref, sin_ref, turn_ref, base):
        deep = outer * BLOCK
        group = max(1, 1024 // deep)
        for g in range(0, both // BLOCK, group):
            at = slice(g * deep, (g + group) * deep)
            part_re = jnp.dot(even_ref[at], cos_ref[...], preferred_element_type=jnp.float32)
            part_im = jnp.dot(odd_ref[at], sin_ref[...], preferred_element_type=jnp.float32)
            for b in range(group):
                re = jnp.zeros((BLOCK, cols), jnp.float32)
                im = jnp.zeros((BLOCK, cols), jnp.float32)
                for s in range(outer):
                    low = b * deep + s * BLOCK
                    re_s = part_re[low : low + BLOCK]
                    im_s = part_im[low : low + BLOCK]
                    cos_s = turn_ref[s : s + 1]
                    sin_s = turn_ref[outer + s : outer + s + 1]
                    re = re + (re_s * cos_s - im_s * sin_s)
                    im = im + (re_s * sin_s + im_s * cos_s)
                low = (g + b) * BLOCK
                for j in range(cols // LANES):
                    at = slice(j * LANES, (j + 1) * LANES)
                    out_ref[base + j, low : low + BLOCK] = re[:, at]
                    out_ref[base + j, both + low : both + low + BLOCK] = im[:, at]

    @pl.when(step == 0)
    def _():
        small[0].start()
        for s in range(outer):
            for copy in copies(s):
                copy.start(priority=1)
        for copy in small[1:]:
            copy.start()
        small[0].wait()
        build(lines_of(0), cos_0, sin_0, turn_0)
        for copy in small[1:]:
            copy.wait()
        start = as_column(start_in, ports, jnp.int32)[:, :1]
        z_ref[...] = as_column(impedance_in, ports, jnp.float32)
        driven_ref[...] = as_column(pairing_in, ports, jnp.int32)
        row = lax.broadcasted_iota(jnp.int32, (FLIP, FLIP), 0)
        col = lax.broadcasted_iota(jnp.int32, (FLIP, FLIP), 1)
        flip = jnp.where(row + col == FLIP - 1, 1.0, 0.0).astype(jnp.bfloat16)
        deep = outer * BLOCK
        group = max(1, 512 // both)
        for g in range(0, outer, group):
            for s in range(g, g + group):
                at = slice(s * inner, (s + 1) * inner)
                time = first + s * inner
                time = time + lax.broadcasted_iota(jnp.int32, (ports, inner), 1)
                keep = time >= start
                for copy in copies(s):
                    copy.wait()
                gated_v = jnp.where(keep, v_in[:, at], 0.0).astype(jnp.bfloat16)
                gated_c = jnp.where(keep, c_in[:, at], 0.0).astype(jnp.bfloat16)
                for b in range(ports // BLOCK):
                    of = slice(b * BLOCK, (b + 1) * BLOCK)
                    low = b * deep + s * BLOCK
                    raw_ref[low : low + BLOCK] = gated_v[of]
                    low += ports // BLOCK * deep
                    raw_ref[low : low + BLOCK] = gated_c[of]
            for b in range(both // BLOCK):
                at = slice(b * deep + g * BLOCK, b * deep + (g + group) * BLOCK)
                for q in range(half // FLIP):
                    to = slice(q * FLIP, (q + 1) * FLIP)
                    behind = jnp.dot(
                        raw_ref[at, half - (q + 1) * FLIP : half - q * FLIP],
                        flip,
                        preferred_element_type=jnp.float32,
                    )
                    ahead = raw_ref[at, half + q * FLIP : half + (q + 1) * FLIP]
                    ahead = ahead.astype(jnp.float32)
                    even_ref[at, to] = (ahead + behind).astype(jnp.bfloat16)
                    odd_ref[at, to] = (ahead - behind).astype(jnp.bfloat16)

    spectra(cos_0, sin_0, turn_0, 0)
    build(lines_of(2 * step + 1), cos_1, sin_1, turn_1)
    spectra(cos_1, sin_1, turn_1, cols // LANES)
    build(lines_of(2 * jnp.minimum(step + 1, steps_count - 1)), cos_0, sin_0, turn_0)


def transform(start, impedance, pairing, freq_index, voltages, currents, total):
    ports, times = voltages.shape
    both = 2 * ports
    count = freq_index.shape[0]
    outer = times // INNER
    half = INNER // 2
    table = pltpu.VMEM((half, COLUMNS), jnp.bfloat16)
    turn = pltpu.VMEM((2 * outer, COLUMNS), jnp.float32)
    column = pl.BlockSpec((ports, LANES), lambda i: (0, 0))
    return pl.pallas_call(
        functools.partial(transform_body, inner=INNER, total=total),
        grid=(count // (2 * COLUMNS),),
        in_specs=[HBM] * 6,
        out_specs=[
            pl.BlockSpec((2 * COLUMNS // LANES, 2 * both, LANES), lambda i: (i, 0, 0)),
            column,
            column,
        ],
        out_shape=[
            pltpu.VMEM((count // LANES, 2 * both, LANES), jnp.float32),
            pltpu.VMEM((ports, LANES), jnp.float32),
            pltpu.VMEM((ports, LANES), jnp.int32),
        ],
        scratch_shapes=[
            pltpu.VMEM((outer * both, half), jnp.bfloat16),
            pltpu.VMEM((outer * both, half), jnp.bfloat16),
            pltpu.VMEM((outer * both, INNER), jnp.bfloat16),
            table,
            table,
            table,
            table,
            turn,
            turn,
            pltpu.VMEM((ports, times), jnp.float32),
            pltpu.VMEM((ports, times), jnp.float32),
            pltpu.VMEM((1, count), jnp.int32),
            pltpu.SMEM((ports,), jnp.int32),
            pltpu.SMEM((ports,), jnp.float32),
            pltpu.SMEM((ports,), jnp.int32),
            pltpu.SemaphoreType.DMA((2, outer)),
            pltpu.SemaphoreType.DMA((4,)),
        ],
        compiler_params=pltpu.CompilerParams(
            dimension_semantics=("arbitrary",), vmem_limit_bytes=48 << 20
        ),
        name="spectrum",
    )(
        in_hbm(start), in_hbm(impedance), in_hbm(pairing), in_hbm(freq_index.reshape(1, count)),
        in_hbm(voltages), in_hbm(currents),
    )


def waves_body(z_ref, parts_ref, sent_ref, own_ref, share_ref, *, scale):
    ports = own_ref.shape[0]
    total = jnp.sum(parts_ref[...], axis=0) * scale
    z = z_ref[...]
    inverse = 1.0 / (2.0 * jnp.sqrt(z))
    power = jnp.zeros((ports, LANES), jnp.float32)
    for r in range(2):
        at = slice(r * LANES, (r + 1) * LANES)
        v = total[2 * r * ports : (2 * r + 1) * ports]
        c = total[(2 * r + 1) * ports : (2 * r + 2) * ports]
        a = (v + z * c) * inverse
        power = power + a * a
        sent_ref[:, at] = a
        own_ref[:, at] = (v - z * c) * inverse
    padded = jnp.concatenate([power, jnp.zeros((LANES - ports, LANES), jnp.float32)], axis=0)
    share = jnp.sum(padded.T, axis=0, keepdims=True)
    share_ref[...] = jnp.broadcast_to(share, share_ref.shape)


def scatter_body(
    driven_ref, same_ref, other_ref, share_0, share_1, share_2, share_3, own_ref, out_ref, *, width
):
    ports = own_ref.shape[0]
    shares = (share_0, share_1, share_2, share_3)
    chips = len(shares)
    place = lax.axis_index("port")
    driven = driven_ref[...]
    holder = driven // ports
    rest = driven % ports
    back = (place // 2 - holder // 2) & (chips - 1)
    core = holder & 1
    lane = lax.broadcasted_iota(jnp.int32, (ports, LANES), 1)
    spot = back * ports + rest
    q = jnp.zeros((ports, 2 * LANES), jnp.float32)
    for swapped, held_ref in enumerate((same_ref, other_ref)):
        here = (lane == spot) & (((place + core) & 1) == swapped)
        picks = jnp.where(here, 1.0, 0.0).astype(jnp.bfloat16)
        left = held_ref[...].reshape(chips * ports, 2 * LANES)
        for _ in range(3):
            term = left.astype(jnp.bfloat16)
            q = q + jnp.dot(picks, term, preferred_element_type=jnp.float32)
            left = left - term.astype(jnp.float32)
    level = jnp.zeros((ports, LANES), jnp.float32)
    sender = lax.broadcasted_iota(jnp.int32, share_0.shape, 0) & 1
    for k in range(chips):
        for c in range(2):
            summed = jnp.where(sender == c, shares[k][...], 0.0)
            summed = jnp.sum(summed, axis=0, keepdims=True)
            level = level + jnp.where((lane == rest) & (back == k) & (core == c), summed, 0.0)
    mean = jnp.sum(level, axis=1, keepdims=True) / width + 1e-06
    q_re, q_im = q[:, :LANES], q[:, LANES:]
    b_re, b_im = own_ref[:, :LANES], own_ref[:, LANES:]
    power = q_re * q_re + q_im * q_im
    inverse = 1.0 / jnp.maximum(power, 0.1 * mean)
    out_ref[0] = (b_re * q_re + b_im * q_im) * inverse
    out_ref[1] = (b_im * q_re - b_re * q_im) * inverse


def body(voltages, currents, impedance, freq_index, window_start, pairing):
    ports, times = voltages.shape
    width = freq_index.shape[0]
    times_count, ports_count = lax.axis_size("tm"), lax.axis_size("port")
    chips = ports_count // 2
    total = times * times_count
    parts, z, driven = transform(
        window_start, impedance, pairing, freq_index, voltages, currents, total
    )
    parts = lax.all_to_all(in_vmem(parts), "tm", 0, 0, tiled=True)
    sent, own, share = pl.pallas_call(
        functools.partial(waves_body, scale=1.0 / math.sqrt(total)),
        in_specs=[VMEM, VMEM],
        out_specs=[VMEM, VMEM, VMEM],
        out_shape=[
            pltpu.VMEM((ports, 2 * LANES), jnp.float32),
            pltpu.VMEM((ports, 2 * LANES), jnp.float32),
            pltpu.VMEM((2 * times_count, LANES), jnp.float32),
        ],
        name="waves",
    )(in_vmem(z), in_vmem(parts))
    columns = [
        [ports_count * t + 2 * x + c for t in range(times_count) for c in range(2)]
        for x in range(chips)
    ]
    ahead = [
        [(i, (i + 2 * k) % ports_count) for i in range(ports_count)] for k in range(1, chips)
    ]
    shares = lax.all_to_all(
        in_vmem(share), ("tm", "port"), 0, 0, tiled=True, axis_index_groups=columns
    )
    along = [sent]
    for k in range(1, chips):
        along.append(lax.ppermute(sent, "port", ahead[k - 1]))
    same = jnp.stack(along)
    other = lax.ppermute(same, "port", [(i, i ^ 1) for i in range(ports_count)])
    means = [shares]
    for k in range(1, chips):
        means.append(lax.ppermute(shares, "port", ahead[k - 1]))
    return pl.pallas_call(
        functools.partial(scatter_body, width=width),
        in_specs=[VMEM] * (chips + 4),
        out_specs=VMEM,
        out_shape=jax.ShapeDtypeStruct((2, ports, LANES), jnp.float32),
        name="scatter",
    )(
        in_vmem(driven), in_vmem(same), in_vmem(other), *map(in_vmem, means), in_vmem(own),
    )


def solution(mesh):
    placed = (P("port", "tm"), P("port", "tm"), P("port"), P(), P("port"), P("port"))
    return jax.shard_map(
        body, mesh=mesh, in_specs=placed, out_specs=P(None, "port", "tm"), check_vma=False
    )
```

```python
import functools
import math

import jax
import jax.numpy as jnp
from jax import lax
from jax.experimental import pallas as pl
from jax.experimental.pallas import tpu as pltpu
from jax.sharding import PartitionSpec as P


LANES = 128
COLUMNS = 256
INNER = 1024
FLIP = 256
BLOCK = 16
VMEM = pl.BlockSpec(memory_space=pltpu.VMEM)
HBM = pl.BlockSpec(memory_space=pltpu.HBM)


def in_hbm(array):
    return pltpu.with_memory_space_constraint(array, pltpu.HBM)


def in_vmem(array):
    return pltpu.with_memory_space_constraint(array, pltpu.VMEM)


def turned(phase, total):
    bits = total.bit_length() - 1
    wrapped = phase & (total - 1)
    quarter = (wrapped + total // 8) >> (bits - 2)
    rest = wrapped - (quarter << (bits - 2))
    x = rest.astype(jnp.float32) * (2.0 * math.pi / total)
    y = x * x
    sine = x + x * y * (-1.6666654611e-1 + y * (8.3321608736e-3 - y * 1.9515295891e-4))
    cosine = (
        1.0
        - 0.5 * y
        + y * y * (4.166664568298827e-2 + y * (-1.388731625493765e-3 + y * 2.443315711809948e-5))
    )
    odd = (quarter & 1) == 1
    even_part = jnp.where(odd, sine, cosine)
    odd_part = jnp.where(odd, cosine, sine)
    flip = ((quarter + 1) & 2) == 2
    below = (quarter & 2) == 2
    return jnp.where(flip, -even_part, even_part), jnp.where(below, odd_part, -odd_part)


def as_column(scalars, rows, dtype):
    row = lax.broadcasted_iota(jnp.int32, (rows, LANES), 0)
    column = jnp.zeros((rows, LANES), dtype)
    for r in range(rows):
        column = jnp.where(row == r, scalars[r], column)
    return column


def transform_body(
    start_ref, impedance_ref, pairing_ref, lines_ref, v_ref, c_ref, out_ref, z_ref, driven_ref,
    even_ref, odd_ref, raw_ref, cos_0, sin_0, cos_1, sin_1, turn_0, turn_1, v_in, c_in, lines_in,
    start_in, impedance_in, pairing_in, sems, small_sems,
    *, inner, total
):
    ports, times = v_ref.shape
    both = 2 * ports
    outer = times // inner
    half = inner // 2
    cols = COLUMNS
    first = lax.axis_index("tm") * times
    step, steps_count = pl.program_id(0), pl.num_programs(0)

    def lines_of(tile):
        return lines_in[:, pl.ds(pl.multiple_of(tile * cols, cols), cols)]

    small = [
        pltpu.make_async_copy(a, b, small_sems.at[n])
        for n, (a, b) in enumerate(
            (
                (lines_ref, lines_in),
                (start_ref, start_in),
                (impedance_ref, impedance_in),
                (pairing_ref, pairing_in),
            )
        )
    ]

    def copies(s):
        at = pl.ds(s * inner, inner)
        return (
            pltpu.make_async_copy(v_ref.at[:, at], v_in.at[:, at], sems.at[0, s]),
            pltpu.make_async_copy(c_ref.at[:, at], c_in.at[:, at], sems.at[1, s]),
        )

    def build(lines, cos_ref, sin_ref, turn_ref):
        def steps(count):
            return lax.broadcasted_iota(jnp.int32, (count, cols), 0)

        fine = 16
        coarse = half // fine
        fine_cos, fine_sin = turned(lines * (2 * steps(fine) + 1), 2 * total)
        near_cos, near_sin = turned(lines * (steps(8) * (2 * fine)), 2 * total)
        far_cos, far_sin = turned(lines * (steps(coarse // 8) * (16 * fine)), 2 * total)
        coarse_cos, coarse_sin = [], []
        for u in range(coarse // 8):
            cos_u, sin_u = far_cos[u : u + 1], far_sin[u : u + 1]
            coarse_cos.append(cos_u * near_cos - sin_u * near_sin)
            coarse_sin.append(sin_u * near_cos + cos_u * near_sin)
        coarse_cos = jnp.concatenate(coarse_cos, axis=0)
        coarse_sin = jnp.concatenate(coarse_sin, axis=0)
        middle = 2 * (first + steps(outer) * inner + half) - 1
        turn_ref[:outer], turn_ref[outer:] = turned(lines * middle, 2 * total)
        for u in range(coarse):
            cos_u, sin_u = coarse_cos[u : u + 1], coarse_sin[u : u + 1]
            at = slice(u * fine, (u + 1) * fine)
            cos_ref[at] = (cos_u * fine_cos - sin_u * fine_sin).astype(jnp.bfloat16)
            sin_ref[at] = (sin_u * fine_cos + cos_u * fine_sin).astype(jnp.bfloat16)

    def spectra(cos_ref, sin_ref, turn_ref, base):
        deep = outer * BLOCK
        group = max(1, 1024 // deep)
        for g in range(0, both // BLOCK, group):
            at = slice(g * deep, (g + group) * deep)
            part_re = jnp.dot(even_ref[at], cos_ref[...], preferred_element_type=jnp.float32)
            part_im = jnp.dot(odd_ref[at], sin_ref[...], preferred_element_type=jnp.float32)
            for b in range(group):
                re = jnp.zeros((BLOCK, cols), jnp.float32)
                im = jnp.zeros((BLOCK, cols), jnp.float32)
                for s in range(outer):
                    low = b * deep + s * BLOCK
                    re_s = part_re[low : low + BLOCK]
                    im_s = part_im[low : low + BLOCK]
                    cos_s = turn_ref[s : s + 1]
                    sin_s = turn_ref[outer + s : outer + s + 1]
                    re = re + (re_s * cos_s - im_s * sin_s)
                    im = im + (re_s * sin_s + im_s * cos_s)
                low = (g + b) * BLOCK
                for j in range(cols // LANES):
                    at = slice(j * LANES, (j + 1) * LANES)
                    out_ref[base + j, low : low + BLOCK] = re[:, at]
                    out_ref[base + j, both + low : both + low + BLOCK] = im[:, at]

    @pl.when(step == 0)
    def _():
        small[0].start()
        for s in range(outer):
            for copy in copies(s):
                copy.start(priority=1)
        for copy in small[1:]:
            copy.start()
        small[0].wait()
        build(lines_of(0), cos_0, sin_0, turn_0)
        for copy in small[1:]:
            copy.wait()
        start = as_column(start_in, ports, jnp.int32)[:, :1]
        z_ref[...] = as_column(impedance_in, ports, jnp.float32)
        driven_ref[...] = as_column(pairing_in, ports, jnp.int32)
        row = lax.broadcasted_iota(jnp.int32, (FLIP, FLIP), 0)
        col = lax.broadcasted_iota(jnp.int32, (FLIP, FLIP), 1)
        flip = jnp.where(row + col == FLIP - 1, 1.0, 0.0).astype(jnp.bfloat16)
        deep = outer * BLOCK
        group = max(1, 512 // both)
        for g in range(0, outer, group):
            for s in range(g, g + group):
                at = slice(s * inner, (s + 1) * inner)
                time = first + s * inner
                time = time + lax.broadcasted_iota(jnp.int32, (ports, inner), 1)
                keep = time >= start
                for copy in copies(s):
                    copy.wait()
                gated_v = jnp.where(keep, v_in[:, at], 0.0).astype(jnp.bfloat16)
                gated_c = jnp.where(keep, c_in[:, at], 0.0).astype(jnp.bfloat16)
                for b in range(ports // BLOCK):
                    of = slice(b * BLOCK, (b + 1) * BLOCK)
                    low = b * deep + s * BLOCK
                    raw_ref[low : low + BLOCK] = gated_v[of]
                    low += ports // BLOCK * deep
                    raw_ref[low : low + BLOCK] = gated_c[of]
            for b in range(both // BLOCK):
                at = slice(b * deep + g * BLOCK, b * deep + (g + group) * BLOCK)
                for q in range(half // FLIP):
                    to = slice(q * FLIP, (q + 1) * FLIP)
                    behind = jnp.dot(
                        raw_ref[at, half - (q + 1) * FLIP : half - q * FLIP],
                        flip,
                        preferred_element_type=jnp.float32,
                    )
                    ahead = raw_ref[at, half + q * FLIP : half + (q + 1) * FLIP]
                    ahead = ahead.astype(jnp.float32)
                    even_ref[at, to] = (ahead + behind).astype(jnp.bfloat16)
                    odd_ref[at, to] = (ahead - behind).astype(jnp.bfloat16)

    spectra(cos_0, sin_0, turn_0, 0)
    build(lines_of(2 * step + 1), cos_1, sin_1, turn_1)
    spectra(cos_1, sin_1, turn_1, cols // LANES)
    build(lines_of(2 * jnp.minimum(step + 1, steps_count - 1)), cos_0, sin_0, turn_0)


def transform(start, impedance, pairing, freq_index, voltages, currents, total):
    ports, times = voltages.shape
    both = 2 * ports
    count = freq_index.shape[0]
    outer = times // INNER
    half = INNER // 2
    table = pltpu.VMEM((half, COLUMNS), jnp.bfloat16)
    turn = pltpu.VMEM((2 * outer, COLUMNS), jnp.float32)
    column = pl.BlockSpec((ports, LANES), lambda i: (0, 0))
    return pl.pallas_call(
        functools.partial(transform_body, inner=INNER, total=total),
        grid=(count // (2 * COLUMNS),),
        in_specs=[HBM] * 6,
        out_specs=[
            pl.BlockSpec((2 * COLUMNS // LANES, 2 * both, LANES), lambda i: (i, 0, 0)),
            column,
            column,
        ],
        out_shape=[
            pltpu.VMEM((count // LANES, 2 * both, LANES), jnp.float32),
            pltpu.VMEM((ports, LANES), jnp.float32),
            pltpu.VMEM((ports, LANES), jnp.int32),
        ],
        scratch_shapes=[
            pltpu.VMEM((outer * both, half), jnp.bfloat16),
            pltpu.VMEM((outer * both, half), jnp.bfloat16),
            pltpu.VMEM((outer * both, INNER), jnp.bfloat16),
            table,
            table,
            table,
            table,
            turn,
            turn,
            pltpu.VMEM((ports, times), jnp.float32),
            pltpu.VMEM((ports, times), jnp.float32),
            pltpu.VMEM((1, count), jnp.int32),
            pltpu.SMEM((ports,), jnp.int32),
            pltpu.SMEM((ports,), jnp.float32),
            pltpu.SMEM((ports,), jnp.int32),
            pltpu.SemaphoreType.DMA((2, outer)),
            pltpu.SemaphoreType.DMA((4,)),
        ],
        compiler_params=pltpu.CompilerParams(
            dimension_semantics=("arbitrary",), vmem_limit_bytes=48 << 20
        ),
        name="spectrum",
    )(
        in_hbm(start), in_hbm(impedance), in_hbm(pairing), in_hbm(freq_index.reshape(1, count)),
        in_hbm(voltages), in_hbm(currents),
    )


def waves_body(z_ref, parts_ref, sent_ref, own_ref, share_ref, *, scale):
    ports = own_ref.shape[0]
    total = jnp.sum(parts_ref[...], axis=0) * scale
    z = z_ref[...]
    inverse = 1.0 / (2.0 * jnp.sqrt(z))
    power = jnp.zeros((ports, LANES), jnp.float32)
    for r in range(2):
        at = slice(r * LANES, (r + 1) * LANES)
        v = total[2 * r * ports : (2 * r + 1) * ports]
        c = total[(2 * r + 1) * ports : (2 * r + 2) * ports]
        a = (v + z * c) * inverse
        power = power + a * a
        sent_ref[:, at] = a
        own_ref[:, at] = (v - z * c) * inverse
    padded = jnp.concatenate([power, jnp.zeros((LANES - ports, LANES), jnp.float32)], axis=0)
    share = jnp.sum(padded.T, axis=0, keepdims=True)
    share_ref[...] = jnp.broadcast_to(share, share_ref.shape)


def pick_body(driven_ref, same_ref, other_ref, own_ref, made_ref):
    ports = own_ref.shape[0]
    chips = same_ref.shape[0]
    place = lax.axis_index("port")
    driven = driven_ref[...]
    holder = driven // ports
    rest = driven % ports
    back = (place // 2 - holder // 2) & (chips - 1)
    core = holder & 1
    lane = lax.broadcasted_iota(jnp.int32, (ports, LANES), 1)
    spot = back * ports + rest
    q = jnp.zeros((ports, 2 * LANES), jnp.float32)
    for swapped, held_ref in enumerate((same_ref, other_ref)):
        here = (lane == spot) & (((place + core) & 1) == swapped)
        picks = jnp.where(here, 1.0, 0.0).astype(jnp.bfloat16)
        left = held_ref[...].reshape(chips * ports, 2 * LANES)
        for _ in range(3):
            term = left.astype(jnp.bfloat16)
            q = q + jnp.dot(picks, term, preferred_element_type=jnp.float32)
            left = left - term.astype(jnp.float32)
    q_re, q_im = q[:, :LANES], q[:, LANES:]
    b_re, b_im = own_ref[:, :LANES], own_ref[:, LANES:]
    made_ref[0] = b_re * q_re + b_im * q_im
    made_ref[1] = b_im * q_re - b_re * q_im
    made_ref[2] = q_re * q_re + q_im * q_im


def scatter_body(driven_ref, share_0, share_1, share_2, share_3, made_ref, out_ref, *, width):
    ports = out_ref.shape[1]
    shares = (share_0, share_1, share_2, share_3)
    chips = len(shares)
    driven = driven_ref[...]
    holder = driven // ports
    rest = driven % ports
    back = (lax.axis_index("port") // 2 - holder // 2) & (chips - 1)
    core = holder & 1
    lane = lax.broadcasted_iota(jnp.int32, (ports, LANES), 1)
    level = jnp.zeros((ports, LANES), jnp.float32)
    sender = lax.broadcasted_iota(jnp.int32, share_0.shape, 0) & 1
    for k in range(chips):
        for c in range(2):
            summed = jnp.where(sender == c, shares[k][...], 0.0)
            summed = jnp.sum(summed, axis=0, keepdims=True)
            level = level + jnp.where((lane == rest) & (back == k) & (core == c), summed, 0.0)
    mean = jnp.sum(level, axis=1, keepdims=True) / width + 1e-06
    inverse = 1.0 / jnp.maximum(made_ref[2], 0.1 * mean)
    out_ref[0] = made_ref[0] * inverse
    out_ref[1] = made_ref[1] * inverse


def body(voltages, currents, impedance, freq_index, window_start, pairing):
    ports, times = voltages.shape
    width = freq_index.shape[0]
    times_count, ports_count = lax.axis_size("tm"), lax.axis_size("port")
    chips = ports_count // 2
    total = times * times_count
    parts, z, driven = transform(
        window_start, impedance, pairing, freq_index, voltages, currents, total
    )
    parts = lax.all_to_all(in_vmem(parts), "tm", 0, 0, tiled=True)
    sent, own, share = pl.pallas_call(
        functools.partial(waves_body, scale=1.0 / math.sqrt(total)),
        in_specs=[VMEM, VMEM],
        out_specs=[VMEM, VMEM, VMEM],
        out_shape=[
            pltpu.VMEM((ports, 2 * LANES), jnp.float32),
            pltpu.VMEM((ports, 2 * LANES), jnp.float32),
            pltpu.VMEM((2 * times_count, LANES), jnp.float32),
        ],
        name="waves",
    )(in_vmem(z), in_vmem(parts))
    columns = [
        [ports_count * t + 2 * x + c for t in range(times_count) for c in range(2)]
        for x in range(chips)
    ]
    ahead = [
        [(i, (i + 2 * k) % ports_count) for i in range(ports_count)] for k in range(1, chips)
    ]
    shares = lax.all_to_all(
        in_vmem(share), ("tm", "port"), 0, 0, tiled=True, axis_index_groups=columns
    )
    along = [sent]
    for k in range(1, chips):
        along.append(lax.ppermute(sent, "port", ahead[k - 1]))
    same = jnp.stack(along)
    other = lax.ppermute(same, "port", [(i, i ^ 1) for i in range(ports_count)])
    means = [shares]
    for k in range(1, chips):
        means.append(lax.ppermute(shares, "port", ahead[k - 1]))
    made = pl.pallas_call(
        pick_body,
        in_specs=[VMEM] * 4,
        out_specs=VMEM,
        out_shape=pltpu.VMEM((3, ports, LANES), jnp.float32),
        name="pick",
    )(in_vmem(driven), in_vmem(same), in_vmem(other), in_vmem(own))
    return pl.pallas_call(
        functools.partial(scatter_body, width=width),
        in_specs=[VMEM] * (chips + 2),
        out_specs=VMEM,
        out_shape=jax.ShapeDtypeStruct((2, ports, LANES), jnp.float32),
        name="scatter",
    )(in_vmem(driven), *map(in_vmem, means), in_vmem(made))


def solution(mesh):
    placed = (P("port", "tm"), P("port", "tm"), P("port"), P(), P("port"), P("port"))
    return jax.shard_map(
        body, mesh=mesh, in_specs=placed, out_specs=P(None, "port", "tm"), check_vma=False
    )
```
